256 devices in a mesh: group: 4 (over z_hi, core), orb: 64 (over x, z_lo, y).
Axes of the slice: x: 4, y: 4, z: 8 (z_hi: 2, z_lo: 4; z = z_hi * 4 + z_lo), core: 2. Of those that a mesh axis runs over, the one named last changes fastest.
Arguments:
- orbitals: bfloat16 [96, 512, 1024], P(None, 'orb'), may hold values from -40 to 40
- potential: float32 [512, 1024], P('orb'), may hold values from -5 to 5
- box_shift: int32 [96], replicated, may hold values from 0 to 31, as said below
- pair_partner: int32 [192, 56], replicated, may hold values from -1 to 1535, as said below
- pair_member: int32 [192, 56], replicated, may hold values from 0 to 7
Outputs:
- hamiltonian: float32 [96, 512, 1024], P(None, 'orb')
The draws below stay inside these ranges and needn't reach their ends.
Inputs may be any that keep to these rules, and one draw needn't show every extreme that they name: Exactly 24 colors have each value of box_shift // 8. `pair_partner`: -1 marks an empty slot; a live slot p of block b names a home orbital of slab (b // 3 + p // 8 - 3) mod (64); some block has every slot live.
All inputs are finite; a program needn't handle non-finite values.
Results may differ from the reference program's by a relative error of at most 0.0004.
Values may be sent and summed in bfloat16 or wider, within the bound.
A program may use at most 128 MiB of HBM per device.

```python
import jax
import jax.numpy as jnp
from jax import lax

B = 32
CX = 8
MEMBERS = 8
QCAP = 8
W = 4
EXCH = 3
HOME = 24
NCOL = 96
NX = 512
PER = 16
NBLK = 192
PCAP = 56


def color_layout(key):
    shuffled = jax.random.permutation(jax.random.fold_in(key, 7), NCOL)
    classes = (shuffled % W).astype(jnp.int32)
    subrows = jax.random.randint(jax.random.fold_in(key, 8), (NCOL,), 0, CX, dtype=jnp.int32)
    return (classes, classes * CX + subrows)


def draw_box_shift(key, part):
    classes, shifts = color_layout(key)
    return shifts.astype(jnp.int32)


def draw_pair_partner(key, part):
    classes, shifts = color_layout(key)
    colors = jnp.arange(NCOL, dtype=jnp.int32)
    color_order = jnp.argsort(classes * NCOL + colors).astype(jnp.int32).reshape(W, HOME)
    slab_total = NX // CX
    block_slab = jnp.arange(NBLK, dtype=jnp.int32) // EXCH
    slot_reach = jnp.arange(PCAP, dtype=jnp.int32) // QCAP - (W - 1)
    partner_slab = (block_slab[:, None] + slot_reach[None, :]) % slab_total
    home_pick = jax.random.randint(jax.random.fold_in(key, 9), (NBLK, PCAP), 0, HOME, dtype=jnp.int32)
    partner_color = color_order[partner_slab % W, home_pick]
    partner_id = partner_color * PER + partner_slab // W
    levels = jax.random.randint(jax.random.fold_in(key, 10), (NBLK,), 0, 101, dtype=jnp.int32)
    cutoff = levels * levels * levels
    full_block = jax.random.randint(jax.random.fold_in(key, 11), (), 0, NBLK, dtype=jnp.int32)
    cutoff = jnp.where(jnp.arange(NBLK, dtype=jnp.int32) == full_block, 1000001, cutoff)
    coin_draws = jax.random.randint(jax.random.fold_in(key, 12), (NBLK, PCAP), 0, 1000000, dtype=jnp.int32)
    return jnp.where(coin_draws < cutoff[:, None], partner_id, -1).astype(jnp.int32)


def smooth_axis(values, axis_no, wrapped):
    reach_cells = 3
    kernel_taps = jnp.exp(-0.5 * jnp.arange(-reach_cells, reach_cells + 1, dtype=jnp.float32) ** 2)
    kernel_taps = kernel_taps / jnp.sqrt(jnp.sum(kernel_taps * kernel_taps))
    length = values.shape[axis_no]
    widths = [(0, 0)] * values.ndim
    widths[axis_no] = (reach_cells, reach_cells)
    padded = jnp.pad(values, widths)
    smoothed = jnp.zeros_like(values)
    for index_no in range(2 * reach_cells + 1):
        offset = index_no - reach_cells
        if wrapped:
            shifted = jnp.roll(values, offset, axis=axis_no)
        else:
            shifted = lax.slice_in_dim(padded, reach_cells - offset, reach_cells - offset + length, axis=axis_no)
        smoothed = smoothed + kernel_taps[index_no] * shifted
    return smoothed


def draw_orbitals(key, part):
    noise_key = jax.random.fold_in(key, 21)
    noise = jax.random.truncated_normal(noise_key, -4.0, 4.0, (NCOL, NX, B, B), jnp.float32)
    color_scale = jnp.ones((NCOL,), jnp.float32)
    smoothed = smooth_axis(noise, 1, True)
    smoothed = smooth_axis(smoothed, 2, False)
    smoothed = smooth_axis(smoothed, 3, False)
    fields = 1.5 * color_scale[:, None, None, None] * smoothed
    return fields.reshape(NCOL, NX, B * B).astype(jnp.bfloat16)


def with_ends(values, key, low, high):
    spot = [jax.random.randint(jax.random.fold_in(key, axis), (), 0, length) for axis, length in enumerate(values.shape)]
    widest = values.shape.index(max(values.shape))
    beside = spot[:widest] + [(spot[widest] + 1) % values.shape[widest]] + spot[widest + 1:]
    return values.at[tuple(spot)].set(low).at[tuple(beside)].set(high)


def block_levels(key, dims, shards, low, high):
    gain, own = 1.0, jax.random.fold_in(key, 6)
    for dim, parts in shards:
        heights = jnp.exp(jax.random.uniform(jax.random.fold_in(own, dim), (parts,), jnp.float32, low / len(shards), high / len(shards)))
        gain = gain * jnp.repeat(heights, dims[dim] // parts).reshape([-1 if axis == dim else 1 for axis in range(len(dims))])
    return gain


def scatter_about(key, dims, spread, most, split=(), kind=jnp.bfloat16):
    result = spread * jax.random.normal(key, dims, jnp.float32)
    if split:
        result = result * block_levels(key, dims, split, -0.22, 0.18)
    return jnp.clip(result, -most, most).astype(kind)


def setup_inputs(seed: int = 0) -> dict:
    arg_keys = jax.random.split(jax.random.key(seed), 6)
    return {
        "orbitals": draw_orbitals(jax.random.fold_in(arg_keys[5], 71), 0),
        "potential": scatter_about(arg_keys[1], (NX, B * B), 1.0, 5.0, ((0, 64),), jnp.float32),
        "box_shift": draw_box_shift(jax.random.fold_in(arg_keys[5], 71), 0),
        "pair_partner": draw_pair_partner(jax.random.fold_in(arg_keys[5], 71), 0),
        "pair_member": with_ends(jax.random.randint(arg_keys[4], (NBLK, PCAP), 0, MEMBERS), jax.random.fold_in(arg_keys[4], 1), 0, MEMBERS - 1).astype(jnp.int32),
    }


lap_weights = (-5369.0 / 1800.0, 12.0 / 7.0, -15.0 / 56.0, 10.0 / 189.0, -1.0 / 112.0, 2.0 / 1925.0, -1.0 / 16632.0)
stencil_reach = 6
mixing = 0.25

def sine_rows(box_edge):
    counter = jnp.arange(1, box_edge + 1, dtype=jnp.float32)
    angles = jnp.pi * counter[:, None] * counter[None, :] / (box_edge + 1)
    return jnp.sqrt(2.0 / (box_edge + 1)) * jnp.sin(angles)

def mode_sums(box_edge):
    counter = jnp.arange(1, box_edge + 1, dtype=jnp.float32)
    single = 2.0 - 2.0 * jnp.cos(jnp.pi * counter / (box_edge + 1))
    cube_sum = single[:, None, None] + single[None, :, None] + single[None, None, :]
    return cube_sum.reshape(box_edge, box_edge * box_edge)

def sine_cube(values, sine_mat):
    box_edge = sine_mat.shape[0]
    for rotation in range(3):
        values = jnp.dot(sine_mat, values, precision=lax.Precision.HIGHEST)
        values = values.reshape(box_edge, box_edge, box_edge).transpose(1, 2, 0).reshape(box_edge, box_edge * box_edge)
    return values

def pair_term(member_box, partner_box, offset, sine_mat, mode_sum):
    box_edge = sine_mat.shape[0]
    padded = jnp.pad(partner_box, ((box_edge, box_edge), (0, 0)))
    shifted = lax.dynamic_slice_in_dim(padded, (box_edge - offset).astype(jnp.int32), box_edge, 0).astype(jnp.float32)
    density = member_box.astype(jnp.float32) * shifted
    solved = sine_cube(sine_cube(density, sine_mat) / mode_sum, sine_mat)
    return -mixing * solved * shifted

def cut_along(padded, axis_no, signed, box_edge):
    starts = [0, stencil_reach, stencil_reach, stencil_reach]
    starts[axis_no] = stencil_reach + signed
    limits = [padded.shape[0]] + [starts[index_no] + box_edge for index_no in (1, 2, 3)]
    return lax.slice(padded, starts, limits)

def second_difference(boxes):
    box_edge = boxes.shape[1]
    padded = jnp.pad(boxes, ((0, 0), (stencil_reach, stencil_reach), (stencil_reach, stencil_reach), (stencil_reach, stencil_reach)))
    summed = 3.0 * lap_weights[0] * boxes
    for offset in range(1, stencil_reach + 1):
        for axis_no in (1, 2, 3):
            summed = summed + lap_weights[offset] * (cut_along(padded, axis_no, offset, box_edge) + cut_along(padded, axis_no, -offset, box_edge))
    return summed

def align_rows(values, row_start):
    doubled = jnp.concatenate([values, values], axis=0)
    return lax.dynamic_slice_in_dim(doubled, row_start.astype(jnp.int32), NX, 0)

def reference(orbitals, potential, box_shift, pair_partner, pair_member):
    starts = box_shift.astype(jnp.int32)

    def local_color(packed):
        orbit_rows, row_start = packed
        aligned = align_rows(orbit_rows, row_start).astype(jnp.float32).reshape(PER, B, B, B)
        field_pot = align_rows(potential, row_start).reshape(PER, B, B, B)
        kinetic = -0.5 * second_difference(aligned)
        return (kinetic + field_pot * aligned).reshape(NX, B * B)
    local_parts = lax.map(local_color, (orbitals, starts))

    def align_color(packed):
        return align_rows(packed[0], packed[1])
    aligned_orbs = lax.map(align_color, (orbitals, starts)).reshape(NCOL, PER, B, B * B)
    classes = box_shift // CX
    color_order = jnp.argsort(classes * NCOL + jnp.arange(NCOL, dtype=jnp.int32)).astype(jnp.int32).reshape(W, HOME)
    flat_partner = pair_partner.reshape(-1)
    flat_member = pair_member.reshape(-1)
    slot_count = NBLK * PCAP
    living = flat_partner >= 0
    slot_order = jnp.argsort(jnp.where(living, 0, 1) * slot_count + jnp.arange(slot_count, dtype=jnp.int32)).astype(jnp.int32)
    live_count = jnp.sum(living.astype(jnp.int32))
    sine_mat = sine_rows(B)
    mode_sum = mode_sums(B)

    def add_pair(counter, accum):
        slot_id = slot_order[counter]
        block_id = slot_id // PCAP
        slab_id = block_id // EXCH
        member_at = block_id % EXCH * MEMBERS + flat_member[slot_id]
        member_color = color_order[slab_id % W, member_at]
        member_index = slab_id // W
        partner = flat_partner[slot_id]
        partner_color = partner // PER
        partner_index = partner % PER
        member_anchor = member_index * B + box_shift[member_color]
        partner_anchor = partner_index * B + box_shift[partner_color]
        offset = (partner_anchor - member_anchor + NX // 2) % NX - NX // 2
        pair_value = pair_term(aligned_orbs[member_color, member_index], aligned_orbs[partner_color, partner_index], offset, sine_mat, mode_sum)
        current = accum[member_color, member_index]
        return accum.at[member_color, member_index].set(current + pair_value)
    exchange = lax.fori_loop(0, live_count, add_pair, jnp.zeros((NCOL, PER, B, B * B), jnp.float32))
    combined = local_parts + exchange.reshape(NCOL, NX, B * B)

    def unalign(packed):
        return align_rows(packed[0], (NX - packed[1]) % NX)
    return lax.map(unalign, (combined, starts))
```

```python
import functools

import jax
import jax.numpy as jnp
import numpy as np
from jax import lax
from jax.experimental import pallas as pl
from jax.experimental.pallas import tpu as pltpu
from jax.sharding import PartitionSpec as P

B = 32
CX = 8
MEMBERS = 8
NCOL = 96
HALF = NCOL // 2
SLABS = 64
WIDTH = 4
CROSS = B * B
QUAD = CROSS // 4
WIN = (WIDTH + 1) * CX
MINE = 12
BATCH = 8
SLOTS = 168

lap_weights = (
    -5369.0 / 1800.0,
    12.0 / 7.0,
    -15.0 / 56.0,
    10.0 / 189.0,
    -1.0 / 112.0,
    2.0 / 1925.0,
    -1.0 / 16632.0,
)
stencil_reach = 6
mixing = 0.25


def halves(values):
    hi = values.astype(jnp.bfloat16).astype(np.float64)
    lo = (values - hi).astype(jnp.bfloat16).astype(np.float64)
    return hi, lo


def tables():
    idx = np.arange(1, B + 1)
    sine = np.sqrt(2.0 / (B + 1)) * np.sin(np.pi * np.outer(idx, idx) / (B + 1))
    single = 2.0 - 2.0 * np.cos(np.pi * idx / (B + 1))
    part = [sine[: B // 2, p::2] for p in (0, 1)]
    lap = np.zeros((B, B))
    for o, w in enumerate(lap_weights):
        lap += w * (np.eye(B, k=o) if o == 0 else np.eye(B, k=o) + np.eye(B, k=-o))
    flip = lap[: B // 2, ::-1][:, : B // 2]
    fold = [lap[: B // 2, : B // 2] + flip, lap[: B // 2, : B // 2] - flip]
    eye = np.eye(B // 2)
    kmat, lmat, modes = [], [], []
    for py in (0, 1):
        for pz in (0, 1):
            kmat.append(np.kron(part[py], part[pz]))
            lmat.append(-0.125 * (np.kron(fold[py], eye) + np.kron(eye, fold[pz])).T)
            cross = single[py::2][:, None] + single[pz::2][None, :]
            modes.append(single[:, None] + cross.reshape(1, -1))
    inv = (-mixing / np.concatenate(modes, axis=1)).astype(np.float32)
    ktab = np.stack(halves(np.stack(kmat))).astype(jnp.bfloat16)
    ltab = np.stack(halves(np.stack(lmat))).astype(jnp.bfloat16)
    a3 = np.zeros((CX, B, 128))
    b3 = np.zeros((CX, WIN, 128))
    lx = np.zeros((CX, WIN, 128))
    for sub in range(CX):
        placed = np.zeros((B, WIN))
        placed[:, sub : sub + B] = sine
        hi, lo = halves(placed)
        a3[sub, :, :120] = np.concatenate([hi, hi, lo], axis=1)
        b3[sub, :, :96] = np.concatenate([hi.T, hi.T, lo.T], axis=1)
        lap_placed = np.zeros((WIN, WIN))
        lap_placed[sub : sub + B, sub : sub + B] = -0.5 * lap
        hi, lo = halves(lap_placed)
        lx[sub, :, :80] = np.concatenate([hi, lo], axis=1)
    return (
        ktab,
        ltab,
        inv,
        a3.astype(np.float32),
        b3.astype(np.float32),
        lx.astype(jnp.bfloat16),
    )


def fold_place(lane):
    y = lane // B
    z = lane % B
    hy = (y >= B // 2).astype(jnp.int32)
    hz = (z >= B // 2).astype(jnp.int32)
    yy = jnp.where(hy == 1, B - 1 - y, y)
    zz = jnp.where(hz == 1, B - 1 - z, z)
    return (hy * 2 + hz) * QUAD + yy * (B // 2) + zz


def butterfly(v):
    q = [v[:, i * QUAD : (i + 1) * QUAD] for i in range(4)]
    sy0, sy1, dy0, dy1 = q[0] + q[2], q[1] + q[3], q[0] - q[2], q[1] - q[3]
    return jnp.concatenate([sy0 + sy1, sy0 - sy1, dy0 + dy1, dy0 - dy1], axis=1)


def split(v):
    hi = v.astype(jnp.bfloat16)
    lo = (v - hi.astype(jnp.float32)).astype(jnp.bfloat16)
    return hi, lo


NT = (((1,), (1,)), ((), ()))
NN = (((1,), (0,)), ((), ()))


def dot3(v, hi_mat, lo_mat, dims):
    hi, lo = split(v)
    f = functools.partial(
        lax.dot_general, dimension_numbers=dims, preferred_element_type=jnp.float32
    )
    return f(hi, hi_mat) + f(lo, hi_mat) + f(hi, lo_mat)


def solve_kernel(
    idx_ref, shift_ref, partner_ref, member_ref,
    own_ref, mine_ref, sib_ref, pot_ref,
    ktab_ref, ltab_ref, inv_ref, a3_ref, b3_ref, lx_ref,
    out_ref,
    wv, acc, stg, pt, home, lm, lci, lcj, lsub, llo,
):
    slab = idx_ref[0]
    core = idx_ref[1]

    def widen(ci, _):
        c_mine = core * HALF + ci
        c_sib = (1 - core) * HALF + ci
        wv[c_mine, 0:CX] = own_ref[c_mine].astype(jnp.float32)
        wv[c_sib, 0:CX] = own_ref[c_sib].astype(jnp.float32)
        for k in range(WIDTH):
            rows = slice((k + 1) * CX, (k + 2) * CX)
            wv[c_mine, rows] = mine_ref[k, ci].astype(jnp.float32)
            wv[c_sib, rows] = sib_ref[k, ci].astype(jnp.float32)
        return 0

    lax.fori_loop(0, HALF, widen, 0)

    def find_home(c, count):
        home[count] = c
        return count + jnp.where(shift_ref[c] // CX == slab % WIDTH, 1, 0)

    lax.fori_loop(0, NCOL, find_home, jnp.int32(0))

    def list_slot(n, count):
        t = n // 56
        pid = partner_ref[n]
        a = t * MEMBERS + member_ref[n]
        live = jnp.logical_and(pid >= 0, a % 2 == core)
        pid = jnp.maximum(pid, 0)
        ci = home[a]
        cj = pid // 16
        rel = ((pid % 16) * B + shift_ref[cj] - slab * CX + 256) & 511
        lm[count] = a // 2
        lci[count] = ci
        lcj[count] = cj
        lsub[count] = shift_ref[ci] % CX
        llo[count] = rel - 256
        return count + jnp.where(live, 1, 0)

    count = lax.fori_loop(0, SLOTS, list_slot, jnp.int32(0))
    for extra in range(BATCH):
        lm[count + extra] = 0
        lci[count + extra] = 0
        lcj[count + extra] = 0
        lsub[count + extra] = 0
        llo[count + extra] = 1000

    row_ids = lax.broadcasted_iota(jnp.int32, (WIN, 1), 0)

    for group in range(2):
        for j in range(6):
            i = group * 6 + j
            c = home[2 * i + core]
            sub = shift_ref[c] % CX
            inside = jnp.logical_and(row_ids >= sub, row_ids < sub + B)
            w = jnp.where(inside, wv[c], 0.0)
            stg[j * WIN : (j + 1) * WIN] = butterfly(w)
            twice = jnp.concatenate([w, w], axis=0).astype(jnp.bfloat16)
            acc[i] = pot_ref[...] * w + jnp.dot(
                lx_ref[sub][:, :80], twice, preferred_element_type=jnp.float32
            )
        for q in range(4):
            cols = slice(q * QUAD, (q + 1) * QUAD)
            v = stg[0 : 6 * WIN, cols]
            stg[0 : 6 * WIN, cols] = dot3(v, ltab_ref[0, q], ltab_ref[1, q], NN)
        for j in range(6):
            i = group * 6 + j
            acc[i] = acc[i] + butterfly(stg[j * WIN : (j + 1) * WIN])

    lane_ids = lax.broadcasted_iota(jnp.int32, (1, 128), 1)
    lane_row = lane_ids - WIN * jnp.where(lane_ids >= WIN, 1, 0)
    lane_row = lane_row - WIN * jnp.where(lane_ids >= 2 * WIN, 1, 0)

    def batch(b, _):
        for p in range(BATCH):
            n = b * BATCH + p
            lo = llo[n]
            held = jnp.logical_and(lane_row >= lo, lane_row < lo + B)
            left = jnp.where(held, a3_ref[lsub[n]], 0.0).astype(jnp.bfloat16)
            dens = wv[lci[n]] * wv[lcj[n]]
            hi = dens.astype(jnp.bfloat16).astype(jnp.float32)
            stack = jnp.concatenate(
                [hi, dens - hi, hi, jnp.zeros((CX, CROSS), jnp.float32)], axis=0
            ).astype(jnp.bfloat16)
            u = jnp.dot(left, stack, preferred_element_type=jnp.float32)
            stg[p * B : (p + 1) * B] = butterfly(u)
        for q in range(4):
            cols = slice(q * QUAD, (q + 1) * QUAD)
            g = dot3(stg[:, cols], ktab_ref[0, q], ktab_ref[1, q], NN)
            g = g.reshape(BATCH, B, QUAD) * inv_ref[:, cols][None]
            g = g.reshape(BATCH * B, QUAD)
            stg[:, cols] = dot3(g, ktab_ref[0, q], ktab_ref[1, q], NT)
        for p in range(BATCH):
            n = b * BATCH + p
            lo = llo[n]
            held = jnp.logical_and(row_ids >= lo, row_ids < lo + B)
            right = jnp.where(held, b3_ref[lsub[n]], 0.0).astype(jnp.bfloat16)
            hi, low = split(butterfly(stg[p * B : (p + 1) * B]))
            stack = jnp.concatenate([hi, low, hi], axis=0)
            field = jnp.dot(right[:, :96], stack, preferred_element_type=jnp.float32)
            m = lm[n]
            acc[m] = acc[m] + field * wv[lcj[n]]
        return 0

    lax.fori_loop(0, (count + BATCH - 1) // BATCH, batch, 0)

    for q in range(4):
        place = fold_place(lax.broadcasted_iota(jnp.int32, (1, QUAD), 1) + q * QUAD)
        rows = lax.broadcasted_iota(jnp.int32, (CROSS, QUAD), 0)
        pt[:, q * QUAD : (q + 1) * QUAD] = jnp.where(rows == place, 1.0, 0.0).astype(
            jnp.bfloat16
        )
    for group in range(2):
        v = acc[group * 6 : group * 6 + 6].reshape(6 * WIN, CROSS)
        hi, lo = split(v)
        for q in range(4):
            cols = slice(q * QUAD, (q + 1) * QUAD)
            y = jnp.dot(hi, pt[:, cols], preferred_element_type=jnp.float32) + jnp.dot(
                lo, pt[:, cols], preferred_element_type=jnp.float32
            )
            for j in range(6):
                for k in range(WIDTH + 1):
                    first = j * WIN + k * CX
                    out_ref[k, group * 6 + j, :, cols] = y[first : first + CX]


def place_kernel(idx_ref, shift_ref, mine_ref, sib_ref, out_ref, rank):
    slab = idx_ref[0]
    core = idx_ref[1]
    for cl in range(WIDTH):
        rank[cl] = 0

    def one(c, _):
        cl = shift_ref[c] // CX
        a = rank[cl]
        rank[cl] = a + 1
        k = (slab - cl) & 3
        i = a // 2
        from_mine = a % 2 == core

        @pl.when(jnp.logical_and(from_mine, k > 0))
        def _():
            out_ref[c] = mine_ref[k, i]

        @pl.when(jnp.logical_and(from_mine, k == 0))
        def _():
            out_ref[c] = mine_ref[0, i] + mine_ref[WIDTH, i]

        @pl.when(jnp.logical_and(jnp.logical_not(from_mine), k > 0))
        def _():
            out_ref[c] = sib_ref[k, i]

        @pl.when(jnp.logical_and(jnp.logical_not(from_mine), k == 0))
        def _():
            out_ref[c] = sib_ref[0, i] + sib_ref[WIDTH, i]

        return 0

    lax.fori_loop(0, NCOL, one, 0)


def forward_route(step):
    pairs = []
    for group in range(4):
        zh, core = group // 2, group % 2
        for s in range(SLABS):
            to = (s + step) % SLABS
            turn = 1 if (s // 4) % 4 == 3 and (to // 4) % 4 == 0 else 0
            there = (zh ^ turn) * 2 + core
            pairs.append((group * SLABS + s, there * SLABS + to))
    return pairs


def ahead(x, step):
    return lax.ppermute(x, ("group", "orb"), forward_route(step))


def behind(x, step):
    return lax.ppermute(x, ("group", "orb"), [(j, i) for i, j in forward_route(step)])


def swap_cores(x):
    return lax.ppermute(x, "group", [(0, 1), (1, 0), (2, 3), (3, 2)])


def body(orbitals, potential, box_shift, pair_partner, pair_member):
    ktab, ltab, inv, a3, b3, lx = tables()
    slab = lax.axis_index("orb").astype(jnp.int32)
    core = lax.axis_index("group").astype(jnp.int32) % 2
    lanes = jnp.arange(CROSS, dtype=jnp.int32)
    fold = (fold_place(lanes)[:, None] == lanes[None, :]).astype(jnp.bfloat16)
    own = jnp.dot(
        orbitals.reshape(NCOL * CX, CROSS), fold, preferred_element_type=jnp.bfloat16
    ).reshape(NCOL, CX, CROSS)
    pot = jnp.dot(
        potential, fold.astype(jnp.float32), precision=lax.Precision.HIGHEST
    )
    half = lax.dynamic_slice_in_dim(own, core * HALF, HALF, 0)
    mine = jnp.stack([behind(half, k) for k in range(1, WIDTH + 1)])
    pots = jnp.concatenate([pot] + [behind(pot, k) for k in range(1, WIDTH + 1)], axis=0)
    sib = swap_cores(mine)
    idx = jnp.stack([slab, core])
    partners = lax.dynamic_slice_in_dim(pair_partner, slab * 3, 3, 0).reshape(-1)
    members = lax.dynamic_slice_in_dim(pair_member, slab * 3, 3, 0).reshape(-1)
    smem = pl.BlockSpec(memory_space=pltpu.SMEM)
    vmem = pl.BlockSpec(memory_space=pltpu.VMEM)
    boxes = pl.pallas_call(
        solve_kernel,
        out_shape=jax.ShapeDtypeStruct((WIDTH + 1, MINE, CX, CROSS), jnp.float32),
        in_specs=[smem] * 4 + [vmem] * 10,
        out_specs=vmem,
        scratch_shapes=[
            pltpu.VMEM((NCOL, WIN, CROSS), jnp.float32),
            pltpu.VMEM((MINE, WIN, CROSS), jnp.float32),
            pltpu.VMEM((BATCH * B, CROSS), jnp.float32),
            pltpu.VMEM((CROSS, CROSS), jnp.bfloat16),
            pltpu.SMEM((32,), jnp.int32),
        ]
        + [pltpu.SMEM((SLOTS + BATCH,), jnp.int32)] * 5,
        compiler_params=pltpu.CompilerParams(vmem_limit_bytes=60 * 2**20),
        name="solve",
    )(idx, box_shift, partners, members, own, mine, sib, pots, ktab, ltab, inv, a3, b3, lx)
    got = jnp.stack([boxes[0]] + [ahead(boxes[k], k) for k in range(1, WIDTH + 1)])
    other = swap_cores(got)
    return pl.pallas_call(
        place_kernel,
        out_shape=jax.ShapeDtypeStruct((NCOL, CX, CROSS), jnp.float32),
        in_specs=[smem] * 2 + [vmem] * 2,
        out_specs=vmem,
        scratch_shapes=[pltpu.SMEM((WIDTH,), jnp.int32)],
        compiler_params=pltpu.CompilerParams(vmem_limit_bytes=40 * 2**20),
        name="place",
    )(idx, box_shift, got, other)


def solution(mesh):
    placed = (P(None, "orb", None), P("orb", None), P(), P(), P())
    return jax.shard_map(
        body, mesh=mesh, in_specs=placed, out_specs=P(None, "orb", None), check_vma=False
    )
```

```python
import functools

import jax
import jax.numpy as jnp
import numpy as np
from jax import lax
from jax.experimental import pallas as pl
from jax.experimental.pallas import tpu as pltpu
from jax.sharding import PartitionSpec as P

B = 32
CX = 8
MEMBERS = 8
NCOL = 96
HALF = NCOL // 2
SLABS = 64
WIDTH = 4
CROSS = B * B
QUAD = CROSS // 4
WIN = (WIDTH + 1) * CX
MINE = 12
BATCH = 8
SLOTS = 168
PIECES = 4
PIECE = HALF // PIECES
SHIPS = 2
BOXES = MINE // SHIPS

lap_weights = (
    -5369.0 / 1800.0,
    12.0 / 7.0,
    -15.0 / 56.0,
    10.0 / 189.0,
    -1.0 / 112.0,
    2.0 / 1925.0,
    -1.0 / 16632.0,
)
stencil_reach = 6
mixing = 0.25


def halves(values):
    hi = values.astype(jnp.bfloat16).astype(np.float64)
    lo = (values - hi).astype(jnp.bfloat16).astype(np.float64)
    return hi, lo


def tables():
    idx = np.arange(1, B + 1)
    sine = np.sqrt(2.0 / (B + 1)) * np.sin(np.pi * np.outer(idx, idx) / (B + 1))
    single = 2.0 - 2.0 * np.cos(np.pi * idx / (B + 1))
    part = [sine[: B // 2, p::2] for p in (0, 1)]
    lap = np.zeros((B, B))
    for o, w in enumerate(lap_weights):
        lap += w * (np.eye(B, k=o) if o == 0 else np.eye(B, k=o) + np.eye(B, k=-o))
    flip = lap[: B // 2, ::-1][:, : B // 2]
    fold = [lap[: B // 2, : B // 2] + flip, lap[: B // 2, : B // 2] - flip]
    eye = np.eye(B // 2)
    kmat, lmat, modes = [], [], []
    for py in (0, 1):
        for pz in (0, 1):
            kmat.append(np.kron(part[py], part[pz]))
            lmat.append(-0.125 * (np.kron(fold[py], eye) + np.kron(eye, fold[pz])).T)
            cross = single[py::2][:, None] + single[pz::2][None, :]
            modes.append(single[:, None] + cross.reshape(1, -1))
    inv = (-mixing / np.concatenate(modes, axis=1)).astype(np.float32)
    ktab = np.stack(halves(np.stack(kmat))).astype(jnp.bfloat16)
    ltab = np.stack(halves(np.stack(lmat))).astype(jnp.bfloat16)
    a3 = np.zeros((CX, B, 128))
    b3 = np.zeros((CX, WIN, 128))
    lx = np.zeros((CX, WIN, 128))
    for sub in range(CX):
        placed = np.zeros((B, WIN))
        placed[:, sub : sub + B] = sine
        hi, lo = halves(placed)
        a3[sub, :, :120] = np.concatenate([hi, hi, lo], axis=1)
        b3[sub, :, :96] = np.concatenate([hi.T, hi.T, lo.T], axis=1)
        lap_placed = np.zeros((WIN, WIN))
        lap_placed[sub : sub + B, sub : sub + B] = -0.5 * lap
        hi, lo = halves(lap_placed)
        lx[sub, :, :80] = np.concatenate([hi, lo], axis=1)
    return (
        ktab,
        ltab,
        inv,
        a3.astype(np.float32),
        b3.astype(np.float32),
        lx.astype(jnp.bfloat16),
    )


def fold_place(lane):
    y = lane // B
    z = lane % B
    hy = (y >= B // 2).astype(jnp.int32)
    hz = (z >= B // 2).astype(jnp.int32)
    yy = jnp.where(hy == 1, B - 1 - y, y)
    zz = jnp.where(hz == 1, B - 1 - z, z)
    return (hy * 2 + hz) * QUAD + yy * (B // 2) + zz


def butterfly(v):
    q = [v[:, i * QUAD : (i + 1) * QUAD] for i in range(4)]
    sy0, sy1, dy0, dy1 = q[0] + q[2], q[1] + q[3], q[0] - q[2], q[1] - q[3]
    return jnp.concatenate([sy0 + sy1, sy0 - sy1, dy0 + dy1, dy0 - dy1], axis=1)


def split(v):
    hi = v.astype(jnp.bfloat16)
    lo = (v - hi.astype(jnp.float32)).astype(jnp.bfloat16)
    return hi, lo


NT = (((1,), (1,)), ((), ()))
NN = (((1,), (0,)), ((), ()))


def dot3(v, hi_mat, lo_mat, dims):
    hi, lo = split(v)
    f = functools.partial(
        lax.dot_general, dimension_numbers=dims, preferred_element_type=jnp.float32
    )
    return f(hi, hi_mat) + f(lo, hi_mat) + f(hi, lo_mat)


def solve_kernel(
    idx_ref, shift_ref, partner_ref, member_ref,
    own_ref, win_ref, pot_ref, potw_ref,
    ktab_ref, ltab_ref, inv_ref, a3_ref, b3_ref, lx_ref,
    out_ref,
    wv, acc, stg, pt, home, lm, lci, lcj, lsub, llo,
):
    slab = idx_ref[0]
    core = idx_ref[1]

    def widen(c, _):
        wv[c, 0:CX] = own_ref[c].astype(jnp.float32)
        for k in range(WIDTH):
            wv[c, (k + 1) * CX : (k + 2) * CX] = win_ref[k, c].astype(jnp.float32)
        return 0

    lax.fori_loop(0, NCOL, widen, 0)
    pots = jnp.concatenate([pot_ref[...], potw_ref[...].reshape(WIDTH * CX, CROSS)], axis=0)

    def find_home(c, count):
        home[count] = c
        return count + jnp.where(shift_ref[c] // CX == slab % WIDTH, 1, 0)

    lax.fori_loop(0, NCOL, find_home, jnp.int32(0))

    def list_slot(n, count):
        t = n // 56
        pid = partner_ref[n]
        a = t * MEMBERS + member_ref[n]
        live = jnp.logical_and(pid >= 0, a % 2 == core)
        pid = jnp.maximum(pid, 0)
        ci = home[a]
        cj = pid // 16
        rel = ((pid % 16) * B + shift_ref[cj] - slab * CX + 256) & 511
        lm[count] = a // 2
        lci[count] = ci
        lcj[count] = cj
        lsub[count] = shift_ref[ci] % CX
        llo[count] = rel - 256
        return count + jnp.where(live, 1, 0)

    count = lax.fori_loop(0, SLOTS, list_slot, jnp.int32(0))
    for extra in range(BATCH):
        lm[count + extra] = 0
        lci[count + extra] = 0
        lcj[count + extra] = 0
        lsub[count + extra] = 0
        llo[count + extra] = 1000

    row_ids = lax.broadcasted_iota(jnp.int32, (WIN, 1), 0)

    for group in range(2):
        for j in range(6):
            i = group * 6 + j
            c = home[2 * i + core]
            sub = shift_ref[c] % CX
            inside = jnp.logical_and(row_ids >= sub, row_ids < sub + B)
            w = jnp.where(inside, wv[c], 0.0)
            stg[j * WIN : (j + 1) * WIN] = butterfly(w)
            twice = jnp.concatenate([w, w], axis=0).astype(jnp.bfloat16)
            acc[i] = pots * w + jnp.dot(
                lx_ref[sub][:, :80], twice, preferred_element_type=jnp.float32
            )
        for q in range(4):
            cols = slice(q * QUAD, (q + 1) * QUAD)
            v = stg[0 : 6 * WIN, cols]
            stg[0 : 6 * WIN, cols] = dot3(v, ltab_ref[0, q], ltab_ref[1, q], NN)
        for j in range(6):
            i = group * 6 + j
            acc[i] = acc[i] + butterfly(stg[j * WIN : (j + 1) * WIN])

    lane_ids = lax.broadcasted_iota(jnp.int32, (1, 128), 1)
    lane_row = lane_ids - WIN * jnp.where(lane_ids >= WIN, 1, 0)
    lane_row = lane_row - WIN * jnp.where(lane_ids >= 2 * WIN, 1, 0)

    def batch(b, _):
        for p in range(BATCH):
            n = b * BATCH + p
            lo = llo[n]
            held = jnp.logical_and(lane_row >= lo, lane_row < lo + B)
            left = jnp.where(held, a3_ref[lsub[n]], 0.0).astype(jnp.bfloat16)
            dens = wv[lci[n]] * wv[lcj[n]]
            hi = dens.astype(jnp.bfloat16).astype(jnp.float32)
            stack = jnp.concatenate(
                [hi, dens - hi, hi, jnp.zeros((CX, CROSS), jnp.float32)], axis=0
            ).astype(jnp.bfloat16)
            u = jnp.dot(left, stack, preferred_element_type=jnp.float32)
            stg[p * B : (p + 1) * B] = butterfly(u)
        for q in range(4):
            cols = slice(q * QUAD, (q + 1) * QUAD)
            g = dot3(stg[:, cols], ktab_ref[0, q], ktab_ref[1, q], NN)
            g = g.reshape(BATCH, B, QUAD) * inv_ref[:, cols][None]
            g = g.reshape(BATCH * B, QUAD)
            stg[:, cols] = dot3(g, ktab_ref[0, q], ktab_ref[1, q], NT)
        for p in range(BATCH):
            n = b * BATCH + p
            lo = llo[n]
            held = jnp.logical_and(row_ids >= lo, row_ids < lo + B)
            right = jnp.where(held, b3_ref[lsub[n]], 0.0).astype(jnp.bfloat16)
            hi, low = split(butterfly(stg[p * B : (p + 1) * B]))
            stack = jnp.concatenate([hi, low, hi], axis=0)
            field = jnp.dot(right[:, :96], stack, preferred_element_type=jnp.float32)
            m = lm[n]
            acc[m] = acc[m] + field * wv[lcj[n]]
        return 0

    lax.fori_loop(0, (count + BATCH - 1) // BATCH, batch, 0)

    for q in range(4):
        place = fold_place(lax.broadcasted_iota(jnp.int32, (1, QUAD), 1) + q * QUAD)
        rows = lax.broadcasted_iota(jnp.int32, (CROSS, QUAD), 0)
        pt[:, q * QUAD : (q + 1) * QUAD] = jnp.where(rows == place, 1.0, 0.0).astype(
            jnp.bfloat16
        )
    for group in range(2):
        v = acc[group * 6 : group * 6 + 6].reshape(6 * WIN, CROSS)
        hi, lo = split(v)
        for q in range(4):
            cols = slice(q * QUAD, (q + 1) * QUAD)
            y = jnp.dot(hi, pt[:, cols], preferred_element_type=jnp.float32) + jnp.dot(
                lo, pt[:, cols], preferred_element_type=jnp.float32
            )
            for j in range(6):
                for k in range(WIDTH + 1):
                    first = j * WIN + k * CX
                    out_ref[k, group * 6 + j, :, cols] = y[first : first + CX]


def place_kernel(idx_ref, shift_ref, mine_ref, sib_ref, got_ref, out_ref, rank):
    slab = idx_ref[0]
    core = idx_ref[1]
    for cl in range(WIDTH):
        rank[cl] = 0

    def one(c, _):
        cl = shift_ref[c] // CX
        a = rank[cl]
        rank[cl] = a + 1
        k = (slab - cl) & 3
        i = a // 2
        side = a % 2

        @pl.when(k > 0)
        def _():
            out_ref[c] = got_ref[k - 1, side, i]

        @pl.when(jnp.logical_and(k == 0, side == core))
        def _():
            out_ref[c] = got_ref[WIDTH - 1, side, i] + mine_ref[i]

        @pl.when(jnp.logical_and(k == 0, side != core))
        def _():
            out_ref[c] = got_ref[WIDTH - 1, side, i] + sib_ref[i]

        return 0

    lax.fori_loop(0, NCOL, one, 0)


def slab_at(step):
    s = lax.axis_index("orb")
    group = lax.axis_index("group")
    y, zl, zh, core = s % 4, (s // 4) % 4, group // 2, group % 2
    if step > 0:
        turn = (zl + (y + step) // 4) // 4
    else:
        turn = 1 - (zl - (1 - (y + step + 4) // 4) + 4) // 4
    return ((zh + turn) % 2 * 2 + core, (s + step + SLABS) % SLABS)


def sibling():
    group = lax.axis_index("group")
    return (group // 2 * 2 + 1 - group % 2, lax.axis_index("orb"))


def greet():
    barrier = pltpu.get_barrier_semaphore()
    others = [slab_at(step) for step in (-4, -3, -2, -1, 1, 2, 3, 4)] + [sibling()]
    for other in others:
        pl.semaphore_signal(
            barrier, inc=1, device_id=other, device_id_type=pl.DeviceIdType.MESH
        )
    pl.semaphore_wait(barrier, len(others))


def remote(src, dst, send, recv, device):
    return pltpu.make_async_remote_copy(
        src_ref=src,
        dst_ref=dst,
        send_sem=send,
        recv_sem=recv,
        device_id=device,
        device_id_type=pl.DeviceIdType.MESH,
    )


def fetch_kernel(own, pot, win, potw, send, recv, dsend, drecv, psend, precv):
    core = lax.axis_index("group") % 2
    y = lax.axis_index("orb") % 4
    greet()

    def part(q):
        return pl.ds(core * HALF + q * PIECE, PIECE)

    def held(k, q):
        return win.at[k - 1, part(q)]

    down, up = slab_at(-1), slab_at(1)
    low, high = slab_at(-3), slab_at(3)

    def move(stream, src, k, q, device):
        return remote(src, held(k, q), send.at[stream, q], recv.at[k - 1, q], device)

    def to_sibling(k, q):
        return remote(
            held(k, q), held(k, q), dsend.at[k - 1, q], drecv.at[k - 1, q], sibling()
        )

    def pot_copy(k):
        return remote(pot, potw.at[k - 1], psend.at[k - 1], precv.at[k - 1], slab_at(-k))

    copies = {
        0: (None, lambda q: move(0, own.at[part(q)], 4, q, slab_at(-4))),
        1: (y >= 1, lambda q: move(1, own.at[part(q)], 1, q, down)),
        2: (y == 3, lambda q: move(2, own.at[part(q)], 3, q, low)),
        3: (y <= 2, lambda q: move(3, held(4, q), 3, q, up)),
        4: (y == 0, lambda q: move(4, held(4, q), 1, q, high)),
        5: ((y == 1) | (y == 2), lambda q: move(5, held(1, q), 2, q, down)),
        6: ((y == 1) | (y == 2), lambda q: move(6, held(3, q), 2, q, up)),
    }

    def act(stream, q, what):
        cond, make = copies[stream]
        if cond is None:
            getattr(make(q), what)()
        else:

            @pl.when(cond)
            def _():
                getattr(make(q), what)()

    def arrived(k, q):
        move(0, held(k, q), k, q, sibling()).wait_recv()
        to_sibling(k, q).start()

    for q in range(PIECES):
        for stream in (0, 1, 2):
            act(stream, q, "start")
    for k in range(1, WIDTH + 1):
        pot_copy(k).start()
    for q in range(PIECES):
        arrived(4, q)
        act(3, q, "start")
        act(4, q, "start")
        arrived(1, q)
        act(5, q, "start")
    for q in range(PIECES):
        arrived(3, q)
        act(6, q, "start")
    for q in range(PIECES):
        arrived(2, q)
    for k in range(1, WIDTH + 1):
        pot_copy(k).wait()
    for q in range(PIECES):
        for stream in range(7):
            act(stream, q, "wait_send")
        for k in range(1, WIDTH + 1):
            to_sibling(k, q).wait()


def spread_kernel(boxes, got, sib0, send, recv, dsend, drecv, osend, orecv):
    core = lax.axis_index("group") % 2
    greet()

    def part(q):
        return pl.ds(q * BOXES, BOXES)

    def ship(k, q):
        return remote(
            boxes.at[k, part(q)],
            got.at[k - 1, core, part(q)],
            send.at[k - 1, q],
            recv.at[k - 1, q],
            slab_at(k),
        )

    def to_sibling(k, q):
        here = got.at[k - 1, core, part(q)]
        return remote(here, here, dsend.at[k - 1, q], drecv.at[k - 1, q], sibling())

    first = remote(boxes.at[0], sib0, osend, orecv, sibling())
    for q in range(SHIPS):
        for k in (4, 1, 3, 2):
            ship(k, q).start()
    first.start()
    for q in range(SHIPS):
        for k in (4, 1, 3, 2):
            ship(k, q).wait_recv()
            to_sibling(k, q).start()
    first.wait()
    for q in range(SHIPS):
        for k in range(1, WIDTH + 1):
            ship(k, q).wait_send()
            to_sibling(k, q).wait()


def body(orbitals, potential, box_shift, pair_partner, pair_member):
    ktab, ltab, inv, a3, b3, lx = tables()
    slab = lax.axis_index("orb").astype(jnp.int32)
    core = lax.axis_index("group").astype(jnp.int32) % 2
    lanes = jnp.arange(CROSS, dtype=jnp.int32)
    fold = (fold_place(lanes)[:, None] == lanes[None, :]).astype(jnp.bfloat16)
    own = jnp.dot(
        orbitals.reshape(NCOL * CX, CROSS), fold, preferred_element_type=jnp.bfloat16
    ).reshape(NCOL, CX, CROSS)
    pot = jnp.dot(
        potential, fold.astype(jnp.float32), precision=lax.Precision.HIGHEST
    )
    smem = pl.BlockSpec(memory_space=pltpu.SMEM)
    vmem = pl.BlockSpec(memory_space=pltpu.VMEM)
    anywhere = pl.BlockSpec(memory_space=pl.ANY)
    dma = pltpu.SemaphoreType.DMA
    win, potw = pl.pallas_call(
        fetch_kernel,
        out_shape=(
            jax.ShapeDtypeStruct((WIDTH, NCOL, CX, CROSS), jnp.bfloat16),
            jax.ShapeDtypeStruct((WIDTH, CX, CROSS), jnp.float32),
        ),
        in_specs=[anywhere] * 2,
        out_specs=(anywhere, anywhere),
        scratch_shapes=[
            dma((7, PIECES)),
            dma((WIDTH, PIECES)),
            dma((WIDTH, PIECES)),
            dma((WIDTH, PIECES)),
            dma((WIDTH,)),
            dma((WIDTH,)),
        ],
        compiler_params=pltpu.CompilerParams(collective_id=0, has_side_effects=True),
        name="fetch",
    )(own, pot)
    idx = jnp.stack([slab, core])
    partners = lax.dynamic_slice_in_dim(pair_partner, slab * 3, 3, 0).reshape(-1)
    members = lax.dynamic_slice_in_dim(pair_member, slab * 3, 3, 0).reshape(-1)
    boxes = pl.pallas_call(
        solve_kernel,
        out_shape=jax.ShapeDtypeStruct((WIDTH + 1, MINE, CX, CROSS), jnp.float32),
        in_specs=[smem] * 4 + [vmem] * 10,
        out_specs=vmem,
        scratch_shapes=[
            pltpu.VMEM((NCOL, WIN, CROSS), jnp.float32),
            pltpu.VMEM((MINE, WIN, CROSS), jnp.float32),
            pltpu.VMEM((BATCH * B, CROSS), jnp.float32),
            pltpu.VMEM((CROSS, CROSS), jnp.bfloat16),
            pltpu.SMEM((32,), jnp.int32),
        ]
        + [pltpu.SMEM((SLOTS + BATCH,), jnp.int32)] * 5,
        compiler_params=pltpu.CompilerParams(vmem_limit_bytes=60 * 2**20),
        name="solve",
    )(idx, box_shift, partners, members, own, win, pot, potw, ktab, ltab, inv, a3, b3, lx)
    piece = (MINE, CX, CROSS)
    got, sib0 = pl.pallas_call(
        spread_kernel,
        out_shape=(
            jax.ShapeDtypeStruct((WIDTH, 2) + piece, jnp.float32),
            jax.ShapeDtypeStruct(piece, jnp.float32),
        ),
        in_specs=[anywhere],
        out_specs=(anywhere, anywhere),
        scratch_shapes=[dma((WIDTH, SHIPS))] * 4 + [dma, dma],
        compiler_params=pltpu.CompilerParams(collective_id=1, has_side_effects=True),
        name="spread",
    )(boxes)
    return pl.pallas_call(
        place_kernel,
        out_shape=jax.ShapeDtypeStruct((NCOL, CX, CROSS), jnp.float32),
        in_specs=[smem] * 2 + [vmem] * 3,
        out_specs=vmem,
        scratch_shapes=[pltpu.SMEM((WIDTH,), jnp.int32)],
        compiler_params=pltpu.CompilerParams(vmem_limit_bytes=40 * 2**20),
        name="place",
    )(idx, box_shift, boxes[0], sib0, got)


def solution(mesh):
    placed = (P(None, "orb", None), P("orb", None), P(), P(), P())
    return jax.shard_map(
        body, mesh=mesh, in_specs=placed, out_specs=P(None, "orb", None), check_vma=False
    )
```

```python
import functools

import jax
import jax.numpy as jnp
import numpy as np
from jax import lax
from jax.experimental import pallas as pl
from jax.experimental.pallas import tpu as pltpu
from jax.sharding import PartitionSpec as P

B = 32
CX = 8
MEMBERS = 8
NCOL = 96
HALF = NCOL // 2
SLABS = 64
WIDTH = 4
CROSS = B * B
QUAD = CROSS // 4
WIN = (WIDTH + 1) * CX
MINE = 12
BATCH = 8
SLOTS = 168
PIECES = 8
PIECE = HALF // PIECES
SHIPS = 4
BOXES = MINE // SHIPS

lap_weights = (
    -5369.0 / 1800.0,
    12.0 / 7.0,
    -15.0 / 56.0,
    10.0 / 189.0,
    -1.0 / 112.0,
    2.0 / 1925.0,
    -1.0 / 16632.0,
)
stencil_reach = 6
mixing = 0.25


def halves(values):
    hi = values.astype(jnp.bfloat16).astype(np.float64)
    lo = (values - hi).astype(jnp.bfloat16).astype(np.float64)
    return hi, lo


def tables():
    idx = np.arange(1, B + 1)
    sine = np.sqrt(2.0 / (B + 1)) * np.sin(np.pi * np.outer(idx, idx) / (B + 1))
    single = 2.0 - 2.0 * np.cos(np.pi * idx / (B + 1))
    part = [sine[: B // 2, p::2] for p in (0, 1)]
    lap = np.zeros((B, B))
    for o, w in enumerate(lap_weights):
        lap += w * (np.eye(B, k=o) if o == 0 else np.eye(B, k=o) + np.eye(B, k=-o))
    flip = lap[: B // 2, ::-1][:, : B // 2]
    fold = [lap[: B // 2, : B // 2] + flip, lap[: B // 2, : B // 2] - flip]
    eye = np.eye(B // 2)
    kmat, lmat, modes = [], [], []
    for py in (0, 1):
        for pz in (0, 1):
            kmat.append(np.kron(part[py], part[pz]))
            lmat.append(-0.125 * (np.kron(fold[py], eye) + np.kron(eye, fold[pz])).T)
            cross = single[py::2][:, None] + single[pz::2][None, :]
            modes.append(single[:, None] + cross.reshape(1, -1))
    inv = (-mixing / np.concatenate(modes, axis=1)).astype(np.float32)
    ktab = np.stack(halves(np.stack(kmat))).astype(jnp.bfloat16)
    ltab = np.stack(halves(np.stack(lmat))).astype(jnp.bfloat16)
    a3 = np.zeros((CX, B, 128))
    b3 = np.zeros((CX, WIN, 128))
    lx = np.zeros((CX, WIN, 128))
    for sub in range(CX):
        placed = np.zeros((B, WIN))
        placed[:, sub : sub + B] = sine
        hi, lo = halves(placed)
        a3[sub, :, :120] = np.concatenate([hi, hi, lo], axis=1)
        b3[sub, :, :96] = np.concatenate([hi.T, hi.T, lo.T], axis=1)
        lap_placed = np.zeros((WIN, WIN))
        lap_placed[sub : sub + B, sub : sub + B] = -0.5 * lap
        hi, lo = halves(lap_placed)
        lx[sub, :, :80] = np.concatenate([hi, lo], axis=1)
    return (
        ktab,
        ltab,
        inv,
        a3.astype(np.float32),
        b3.astype(np.float32),
        lx.astype(jnp.bfloat16),
    )


def fold_lane(j, hy):
    hz, yp, zp = j // 128, j % 128 // 16, j % 16
    yl = yp if hy == 0 else 7 - yp
    return yl * B + zp + hz * (B - 1 - 2 * zp)


def folding(hy):
    j = lax.broadcasted_iota(jnp.int32, (1, QUAD), 1)
    lanes = lax.broadcasted_iota(jnp.int32, (QUAD, QUAD), 0)
    return jnp.where(lanes == fold_lane(j, hy), 1.0, 0.0).astype(jnp.bfloat16)


def unfolding(hy):
    j = lax.broadcasted_iota(jnp.int32, (QUAD, 1), 0)
    lanes = lax.broadcasted_iota(jnp.int32, (QUAD, QUAD), 1)
    return jnp.where(lanes == fold_lane(j, hy), 1.0, 0.0).astype(jnp.bfloat16)


def chunk_home(n):
    hy = n // 2
    h = n if hy == 0 else 3 - n
    return [slice((hy * 2 + hz) * QUAD + h * 128, (hy * 2 + hz) * QUAD + h * 128 + 128) for hz in (0, 1)]


def butterfly(v):
    q = [v[:, i * QUAD : (i + 1) * QUAD] for i in range(4)]
    sy0, sy1, dy0, dy1 = q[0] + q[2], q[1] + q[3], q[0] - q[2], q[1] - q[3]
    return jnp.concatenate([sy0 + sy1, sy0 - sy1, dy0 + dy1, dy0 - dy1], axis=1)


def split(v):
    hi = v.astype(jnp.bfloat16)
    lo = (v - hi.astype(jnp.float32)).astype(jnp.bfloat16)
    return hi, lo


def dot3(v, hi_mat, lo_mat):
    hi, lo = split(v)
    rows = v.shape[0]
    both = jnp.dot(
        jnp.concatenate([hi, lo], axis=0), hi_mat, preferred_element_type=jnp.float32
    )
    low = jnp.dot(hi, lo_mat, preferred_element_type=jnp.float32)
    return both[:rows] + both[rows:] + low


GROUP = 32


def prep_kernel(orb_ref, pot_ref, own_ref, planes_ref):
    fold = [folding(0), folding(1)]

    def some(g, _):
        x = orb_ref[pl.ds(g * GROUP, GROUP)].astype(jnp.float32)
        x = x.reshape(GROUP * CX, CROSS).astype(jnp.bfloat16)
        for n in range(4):
            y = jnp.dot(
                x[:, n * QUAD : (n + 1) * QUAD],
                fold[n // 2],
                preferred_element_type=jnp.float32,
            )
            for hz, lanes in enumerate(chunk_home(n)):
                part = y[:, hz * 128 : hz * 128 + 128].reshape(GROUP, CX, 128)
                own_ref[pl.ds(g * GROUP, GROUP), :, lanes] = part.astype(jnp.bfloat16)
        return 0

    lax.fori_loop(0, NCOL // GROUP, some, 0)
    rest = pot_ref[...]
    planes = []
    for _ in range(3):
        top = rest.astype(jnp.bfloat16).astype(jnp.float32)
        planes.append(top)
        rest = rest - top
    x = jnp.concatenate(planes + [jnp.zeros_like(rest)], axis=0).astype(jnp.bfloat16)
    for n in range(4):
        y = jnp.dot(
            x[:, n * QUAD : (n + 1) * QUAD], fold[n // 2], preferred_element_type=jnp.float32
        )
        for hz, lanes in enumerate(chunk_home(n)):
            for p in range(4):
                part = y[p * CX : (p + 1) * CX, hz * 128 : hz * 128 + 128]
                planes_ref[p // 2, p % 2, :, lanes] = part.astype(jnp.bfloat16)


def solve_kernel(
    idx_ref, shift_ref, partner_ref, member_ref,
    own_hbm, win_hbm, pot_ref, potw_ref,
    ktab_hbm, ltab_hbm, inv_ref, a3_ref, b3_ref, lx_ref,
    out_ref,
    own_ref, win_ref, ktab_ref, ltab_ref, ktr_ref,
    wv, pots, acc, stg, home, listed, sems,
):
    slab = idx_ref[0]
    core = idx_ref[1]
    loads = [
        pltpu.make_async_copy(own_hbm, own_ref, sems.at[0]),
        *(
            pltpu.make_async_copy(win_hbm.at[k], win_ref.at[k], sems.at[1 + k])
            for k in range(WIDTH)
        ),
        pltpu.make_async_copy(ltab_hbm, ltab_ref, sems.at[WIDTH + 1]),
        pltpu.make_async_copy(ktab_hbm, ktab_ref, sems.at[WIDTH + 2]),
    ]
    for load in loads:
        load.start()

    def find_home(c, count):
        home[count] = c
        return count + jnp.where((shift_ref[c] >> 3) == (slab & 3), 1, 0)

    lax.fori_loop(0, NCOL, find_home, jnp.int32(0), unroll=8)
    base = 256 - slab * CX

    count = jnp.int32(0)
    for t in range(3):
        block = slab * 3 + t

        def list_slot(p, count, t=t, block=block):
            pid = partner_ref[p, block]
            a = t * MEMBERS + member_ref[p, block]
            live = jnp.logical_and(pid >= 0, (a & 1) == core)
            pid = jnp.maximum(pid, 0)
            cj = pid >> 4
            rel = (((pid & 15) << 5) + shift_ref[cj] + base) & 511
            listed[count] = ((rel - 224) << 19) + (cj << 12) + (home[a] << 5) + a
            return count + jnp.where(live, 1, 0)

        count = lax.fori_loop(0, SLOTS // 3, list_slot, count, unroll=8)
    for extra in range(BATCH):
        listed[count + extra] = 1024 << 19

    def pair(n):
        word = listed[n]
        ci = (word >> 5) & 127
        return (word >> 1) & 15, ci, (word >> 12) & 127, shift_ref[ci] & 7, (word >> 19) - 32

    lead = idx_ref[2] * WIDTH * CX
    lead_rows = pl.ds(pl.multiple_of(lead, CX), CX)
    tail_rows = pl.ds(pl.multiple_of(WIDTH * CX - lead, CX), CX)

    def whole(planes):
        f = jnp.float32
        return planes[0, 0].astype(f) + planes[0, 1].astype(f) + planes[1, 0].astype(f)

    pots[lead_rows] = whole(pot_ref)
    pots[tail_rows] = whole(potw_ref.at[WIDTH - 1])
    for k in range(1, WIDTH):
        pots[k * CX : (k + 1) * CX] = whole(potw_ref.at[k - 1])

    def widen(rows, source):
        def one(c, _):
            wv[c, rows] = source[c].astype(jnp.float32)
            return 0

        lax.fori_loop(0, NCOL, one, 0, unroll=4)

    loads[0].wait()
    widen(lead_rows, own_ref)
    for k in range(WIDTH):
        loads[1 + k].wait()
        rows = tail_rows if k == WIDTH - 1 else slice((k + 1) * CX, (k + 2) * CX)
        widen(rows, win_ref.at[k])
    loads[WIDTH + 1].wait()
    loads[WIDTH + 2].wait()
    for h in range(2):
        for q in range(4):
            ktr_ref[h, q] = ktab_ref[h, q].astype(jnp.float32).T.astype(jnp.bfloat16)

    row_ids = lax.broadcasted_iota(jnp.int32, (WIN, 1), 0)

    for group in range(2):
        for j in range(6):
            i = group * 6 + j
            c = home[2 * i + core]
            sub = shift_ref[c] % CX
            inside = jnp.logical_and(row_ids >= sub, row_ids < sub + B)
            w = jnp.where(inside, wv[c], 0.0)
            stg[j * WIN : (j + 1) * WIN] = butterfly(w)
            twice = jnp.concatenate([w, w], axis=0).astype(jnp.bfloat16)
            acc[i] = pots[...] * w + jnp.dot(
                lx_ref[sub][:, :80], twice, preferred_element_type=jnp.float32
            )
        for q in range(4):
            cols = slice(q * QUAD, (q + 1) * QUAD)
            v = stg[0 : 6 * WIN, cols]
            stg[0 : 6 * WIN, cols] = dot3(v, ltab_ref[0, q], ltab_ref[1, q])
        for j in range(6):
            i = group * 6 + j
            acc[i] = acc[i] + butterfly(stg[j * WIN : (j + 1) * WIN])

    lane_ids = lax.broadcasted_iota(jnp.int32, (1, 128), 1)
    lane_row = lane_ids - WIN * jnp.where(lane_ids >= WIN, 1, 0)
    lane_row = lane_row - WIN * jnp.where(lane_ids >= 2 * WIN, 1, 0)

    def batch(b, _):
        for p in range(BATCH):
            _, ci, cj, sub, lo = pair(b * BATCH + p)
            held = jnp.logical_and(lane_row >= lo, lane_row < lo + B)
            left = jnp.where(held, a3_ref[sub], 0.0).astype(jnp.bfloat16)
            dens = wv[ci] * wv[cj]
            hi = dens.astype(jnp.bfloat16).astype(jnp.float32)
            stack = jnp.concatenate(
                [hi, dens - hi, hi, jnp.zeros((CX, CROSS), jnp.float32)], axis=0
            ).astype(jnp.bfloat16)
            u = jnp.dot(left, stack, preferred_element_type=jnp.float32)
            stg[p * B : (p + 1) * B] = butterfly(u)
        for q in range(4):
            cols = slice(q * QUAD, (q + 1) * QUAD)
            g = dot3(stg[:, cols], ktab_ref[0, q], ktab_ref[1, q])
            g = g.reshape(BATCH, B, QUAD) * inv_ref[:, cols][None]
            g = g.reshape(BATCH * B, QUAD)
            stg[:, cols] = dot3(g, ktr_ref[0, q], ktr_ref[1, q])
        for p in range(BATCH):
            m, _, cj, sub, lo = pair(b * BATCH + p)
            held = jnp.logical_and(row_ids >= lo, row_ids < lo + B)
            right = jnp.where(held, b3_ref[sub], 0.0).astype(jnp.bfloat16)
            hi, low = split(butterfly(stg[p * B : (p + 1) * B]))
            stack = jnp.concatenate([hi, low, hi], axis=0)
            field = jnp.dot(right[:, :96], stack, preferred_element_type=jnp.float32)
            acc[m] = acc[m] + field * wv[cj]
        return 0

    lax.fori_loop(0, (count + BATCH - 1) // BATCH, batch, 0)

    for n in range(4):
        back = unfolding(n // 2)
        low_z, high_z = chunk_home(n)
        for group in range(2):
            rows = slice(group * 6, group * 6 + 6)
            v = jnp.concatenate([acc[rows, :, low_z], acc[rows, :, high_z]], axis=2)
            hi, lo = split(v.reshape(6 * WIN, QUAD))
            y = jnp.dot(
                jnp.concatenate([hi, lo], axis=0), back, preferred_element_type=jnp.float32
            )
            y = y[: 6 * WIN] + y[6 * WIN :]
            for j in range(6):
                for k in range(WIDTH + 1):
                    first = j * WIN + k * CX
                    out_ref[k, group * 6 + j, :, n * QUAD : (n + 1) * QUAD] = y[
                        first : first + CX
                    ]


def slab_at(step):
    s = lax.axis_index("orb")
    group = lax.axis_index("group")
    y, zl, zh, core = s % 4, (s // 4) % 4, group // 2, group % 2
    if step > 0:
        turn = (zl + (y + step) // 4) // 4
    else:
        turn = 1 - (zl - (1 - (y + step + 4) // 4) + 4) // 4
    return ((zh + turn) % 2 * 2 + core, (s + step + SLABS) % SLABS)


def ring(step):
    s = lax.axis_index("orb")
    return (lax.axis_index("group"), s - s % 4 + (s % 4 + step + 4) % 4)


def either(which, first, second):
    return tuple(a + which * (b - a) for a, b in zip(first, second))


def sibling():
    group = lax.axis_index("group")
    return (group // 2 * 2 + 1 - group % 2, lax.axis_index("orb"))


def greet(others):
    barrier = pltpu.get_barrier_semaphore()
    for other in others:
        pl.semaphore_signal(
            barrier, inc=1, device_id=other, device_id_type=pl.DeviceIdType.MESH
        )
    pl.semaphore_wait(barrier, len(others))


def remote(src, dst, send, recv, device):
    return pltpu.make_async_remote_copy(
        src_ref=src,
        dst_ref=dst,
        send_sem=send,
        recv_sem=recv,
        device_id=device,
        device_id_type=pl.DeviceIdType.MESH,
    )


def fetch_kernel(own, pot, win, potw, send, recv, dsend, drecv):
    core = lax.axis_index("group") % 2
    y = lax.axis_index("orb") % 4
    high, odd = y // 2, y % 2
    greet([ring(-1), ring(1), slab_at(-4), slab_at(4), sibling()])

    def mine(q):
        return pot.at[core] if q == PIECES else own.at[pl.ds(core * HALF + q * PIECE, PIECE)]

    def held(t, q):
        if q == PIECES:
            return potw.at[t, core]
        return win.at[t, pl.ds(core * HALF + q * PIECE, PIECE)]

    def move(stream, src, t, q, device):
        return remote(src, held(t, q), send.at[stream, q], recv.at[t, q], device)

    def to_sibling(t, q):
        return remote(held(t, q), held(t, q), dsend.at[t, q], drecv.at[t, q], sibling())

    relayed = 2 - 2 * odd
    onward = either(odd, ring(1), ring(-1))
    copies = {
        0: (None, lambda q: move(0, mine(q), 3, q, either(high, slab_at(-4), slab_at(4)))),
        1: (y != 3, lambda q: move(1, mine(q), 0, q, ring(-1))),
        2: (y == 3, lambda q: move(1, held(3, q), 0, q, ring(-1))),
        3: (y != 0, lambda q: move(2, mine(q), 2, q, ring(1))),
        4: (y == 0, lambda q: move(2, held(3, q), 2, q, ring(1))),
        5: (None, lambda q: move(3, held(relayed, q), 1, q, onward)),
    }

    def act(which, q, what):
        cond, make = copies[which]
        if cond is None:
            getattr(make(q), what)()
        else:

            @pl.when(cond)
            def _():
                getattr(make(q), what)()

    def arrived(t, q):
        move(0, held(t, q), t, q, sibling()).wait_recv()
        to_sibling(t, q).start()

    turns = range(PIECES + 1)
    for q in turns:
        for which in (0, 1, 3):
            act(which, q, "start")
    for q in turns:
        arrived(3, q)
        act(2, q, "start")
        act(4, q, "start")
        arrived(relayed, q)
        act(5, q, "start")
    for q in turns:
        arrived(2 - relayed, q)
    for q in turns:
        arrived(1, q)
    for q in turns:
        for which in range(6):
            act(which, q, "wait_send")
        for t in range(WIDTH):
            to_sibling(t, q).wait()


def spread_kernel(
    shift_ref, boxes, out, got, ext, stage,
    send, recv, rsend, rrecv, dsend, drecv, osend, orecv, ksem,
):
    core = lax.axis_index("group") % 2
    slab = lax.axis_index("orb")
    y = slab % 4
    high, odd = y // 2, y % 2
    greet(
        [ring(-1), ring(1), slab_at(-4), slab_at(4), slab_at(-3), slab_at(3), sibling()]
    )

    def part(q):
        return pl.ds(q * BOXES, BOXES)

    def ship(t, src, q, device):
        return remote(
            src, got.at[t, core, part(q)], send.at[t, q], recv.at[t, q], device
        )

    low_cross = (y % 2) * (1 - high)
    high_cross = (1 - y % 2) * high
    to_one = either(high_cross, ring(1), slab_at(-3))
    to_three = either(low_cross, ring(-1), slab_at(3))
    to_z = either(high, slab_at(4), slab_at(-4))
    outer = WIDTH * (1 - high)
    inner = WIDTH * high

    def by_z(q):
        return ship(3, boxes.at[outer, part(q)], q, to_z)

    def by_one(q):
        return ship(0, boxes.at[1, part(q)], q, to_one)

    def by_three(q):
        return ship(2, boxes.at[3, part(q)], q, to_three)

    def to_relay(q):
        return remote(
            boxes.at[2, part(q)],
            stage.at[part(q)],
            rsend.at[q],
            rrecv.at[q],
            either(odd, ring(1), ring(-1)),
        )

    def relay(q):
        return ship(1, stage.at[part(q)], q, either(odd, ring(-1), ring(1)))

    def to_sibling(t, q):
        here = got.at[t, core, part(q)]
        return remote(here, here, dsend.at[t, q], drecv.at[t, q], sibling())

    def arrived(t, q):
        ship(t, boxes.at[0, part(q)], q, sibling()).wait_recv()
        to_sibling(t, q).start()

    local = remote(boxes.at[inner], ext.at[core], osend, orecv, sibling())
    for q in range(SHIPS):
        to_relay(q).start()
    for q in range(SHIPS):
        by_z(q).start()
        by_one(q).start()
        by_three(q).start()
    local.start()
    keep = pltpu.make_async_copy(boxes.at[inner], ext.at[core], ksem)
    keep.start()
    for q in range(SHIPS):
        to_relay(q).wait_recv()
        relay(q).start()
    for q in range(SHIPS):
        arrived(3, q)
        arrived(0, q)
        arrived(2, q)
    for q in range(SHIPS):
        arrived(1, q)
    local.wait()
    keep.wait()
    for q in range(SHIPS):
        to_relay(q).wait_send()
        for copy in (by_z(q), by_one(q), by_three(q), relay(q)):
            copy.wait_send()
        for t in range(WIDTH):
            to_sibling(t, q).wait()

    def place(c, ranks):
        cl = shift_ref[c] // CX
        a = sum(jnp.where(cl == n, rank, 0) for n, rank in enumerate(ranks))
        a = jnp.minimum(a, 2 * MINE - 1)
        k = (slab - cl + SLABS) % 4
        t = jnp.where(k == 0, WIDTH - 1, k - 1)
        extra = jnp.where(k == 0, 1.0, 0.0)
        out[c] = got[t, a % 2, a // 2] + extra * ext[a % 2, a // 2]
        return tuple(rank + jnp.where(cl == n, 1, 0) for n, rank in enumerate(ranks))

    lax.fori_loop(0, NCOL, place, (jnp.int32(0),) * WIDTH, unroll=4)


def body(orbitals, potential, box_shift, pair_partner, pair_member):
    ktab, ltab, inv, a3, b3, lx = tables()
    place = lax.axis_index("orb").astype(jnp.int32)
    high = place % 4 // 2
    slab = (place - 4 * high) % SLABS
    core = lax.axis_index("group").astype(jnp.int32) % 2
    smem = pl.BlockSpec(memory_space=pltpu.SMEM)
    vmem = pl.BlockSpec(memory_space=pltpu.VMEM)
    hbm = pl.BlockSpec(memory_space=pltpu.HBM)
    dma = pltpu.SemaphoreType.DMA
    own, pot = pl.pallas_call(
        prep_kernel,
        out_shape=(
            jax.ShapeDtypeStruct((NCOL, CX, CROSS), jnp.bfloat16),
            jax.ShapeDtypeStruct((2, 2, CX, CROSS), jnp.bfloat16),
        ),
        in_specs=[vmem] * 2,
        out_specs=(vmem, vmem),
        name="prep",
    )(orbitals, potential)
    streams = (WIDTH, PIECES + 1)
    win, potw = pl.pallas_call(
        fetch_kernel,
        out_shape=(
            jax.ShapeDtypeStruct((WIDTH, NCOL, CX, CROSS), jnp.bfloat16),
            jax.ShapeDtypeStruct((WIDTH, 2, 2, CX, CROSS), jnp.bfloat16),
        ),
        in_specs=[hbm] * 2,
        out_specs=(hbm, hbm),
        scratch_shapes=[dma(streams)] * 4,
        compiler_params=pltpu.CompilerParams(collective_id=0, has_side_effects=True),
        name="fetch",
    )(own, pot)
    idx = jnp.stack([slab, core, high])
    boxes = pl.pallas_call(
        solve_kernel,
        out_shape=jax.ShapeDtypeStruct((WIDTH + 1, MINE, CX, CROSS), jnp.float32),
        in_specs=[smem] * 4 + [hbm] * 2 + [vmem] * 2 + [hbm] * 2 + [vmem] * 4,
        out_specs=vmem,
        scratch_shapes=[
            pltpu.VMEM((NCOL, CX, CROSS), jnp.bfloat16),
            pltpu.VMEM((WIDTH, NCOL, CX, CROSS), jnp.bfloat16),
        ]
        + [pltpu.VMEM((2, 4, QUAD, QUAD), jnp.bfloat16)] * 3
        + [
            pltpu.VMEM((NCOL, WIN, CROSS), jnp.float32),
            pltpu.VMEM((WIN, CROSS), jnp.float32),
            pltpu.VMEM((MINE, WIN, CROSS), jnp.float32),
            pltpu.VMEM((BATCH * B, CROSS), jnp.float32),
            pltpu.SMEM((32,), jnp.int32),
        ]
        + [pltpu.SMEM((SLOTS + BATCH,), jnp.int32)]
        + [dma((WIDTH + 3,))],
        compiler_params=pltpu.CompilerParams(vmem_limit_bytes=60 * 2**20),
        name="solve",
    )(idx, box_shift, pair_partner.T, pair_member.T, own, win, pot, potw, ktab, ltab, inv, a3, b3, lx)
    piece = (MINE, CX, CROSS)
    ships = (WIDTH, SHIPS)
    return pl.pallas_call(
        spread_kernel,
        out_shape=jax.ShapeDtypeStruct((NCOL, CX, CROSS), jnp.float32),
        in_specs=[smem, hbm],
        out_specs=vmem,
        scratch_shapes=[
            pltpu.VMEM((WIDTH, 2) + piece, jnp.float32),
            pltpu.VMEM((2,) + piece, jnp.float32),
            pltpu.VMEM(piece, jnp.float32),
            dma(ships),
            dma(ships),
            dma((SHIPS,)),
            dma((SHIPS,)),
            dma(ships),
            dma(ships),
            dma,
            dma,
            dma,
        ],
        compiler_params=pltpu.CompilerParams(
            collective_id=1, has_side_effects=True, vmem_limit_bytes=40 * 2**20
        ),
        name="spread",
    )(box_shift, boxes)


def solution(mesh):
    placed = (P(None, "orb", None), P("orb", None), P(), P(), P())
    return jax.shard_map(
        body, mesh=mesh, in_specs=placed, out_specs=P(None, "orb", None), check_vma=False
    )
```

```python
import functools

import jax
import jax.numpy as jnp
import numpy as np
from jax import lax
from jax.experimental import pallas as pl
from jax.experimental.pallas import tpu as pltpu
from jax.sharding import PartitionSpec as P

B = 32
CX = 8
MEMBERS = 8
NCOL = 96
HALF = NCOL // 2
SLABS = 64
WIDTH = 4
CROSS = B * B
QUAD = CROSS // 4
WIN = (WIDTH + 1) * CX
MINE = 12
BATCH = 8
SLOTS = 168
PIECES = 8
PIECE = HALF // PIECES
SHIPS = 4
BOXES = MINE // SHIPS

lap_weights = (
    -5369.0 / 1800.0,
    12.0 / 7.0,
    -15.0 / 56.0,
    10.0 / 189.0,
    -1.0 / 112.0,
    2.0 / 1925.0,
    -1.0 / 16632.0,
)
stencil_reach = 6
mixing = 0.25


def halves(values):
    hi = values.astype(jnp.bfloat16).astype(np.float64)
    lo = (values - hi).astype(jnp.bfloat16).astype(np.float64)
    return hi, lo


def tables():
    idx = np.arange(1, B + 1)
    sine = np.sqrt(2.0 / (B + 1)) * np.sin(np.pi * np.outer(idx, idx) / (B + 1))
    single = 2.0 - 2.0 * np.cos(np.pi * idx / (B + 1))
    part = [sine[: B // 2, p::2] for p in (0, 1)]
    lap = np.zeros((B, B))
    for o, w in enumerate(lap_weights):
        lap += w * (np.eye(B, k=o) if o == 0 else np.eye(B, k=o) + np.eye(B, k=-o))
    flip = lap[: B // 2, ::-1][:, : B // 2]
    fold = [lap[: B // 2, : B // 2] + flip, lap[: B // 2, : B // 2] - flip]
    eye = np.eye(B // 2)
    kmat, lmat, modes = [], [], []
    for py in (0, 1):
        for pz in (0, 1):
            kmat.append(np.kron(part[py], part[pz]))
            lmat.append(-0.125 * (np.kron(fold[py], eye) + np.kron(eye, fold[pz])).T)
            cross = single[py::2][:, None] + single[pz::2][None, :]
            modes.append(single[:, None] + cross.reshape(1, -1))
    inv = (-mixing / np.concatenate(modes, axis=1)).astype(np.float32)
    ktab = np.stack(halves(np.stack(kmat))).astype(jnp.bfloat16)
    ltab = np.stack(halves(np.stack(lmat))).astype(jnp.bfloat16)
    a3 = np.zeros((CX, B, 128))
    b3 = np.zeros((CX, WIN, 128))
    lx = np.zeros((CX, WIN, 128))
    for sub in range(CX):
        placed = np.zeros((B, WIN))
        placed[:, sub : sub + B] = sine
        hi, lo = halves(placed)
        a3[sub, :, :120] = np.concatenate([hi, hi, lo], axis=1)
        b3[sub, :, :96] = np.concatenate([hi.T, hi.T, lo.T], axis=1)
        lap_placed = np.zeros((WIN, WIN))
        lap_placed[sub : sub + B, sub : sub + B] = -0.5 * lap
        hi, lo = halves(lap_placed)
        lx[sub, :, :80] = np.concatenate([hi, lo], axis=1)
    return (
        ktab,
        ltab,
        inv,
        a3.astype(np.float32),
        b3.astype(np.float32),
        lx.astype(jnp.bfloat16),
    )


def fold_lane(j, hy):
    hz, yp, zp = j // 128, j % 128 // 16, j % 16
    yl = yp if hy == 0 else 7 - yp
    return yl * B + zp + hz * (B - 1 - 2 * zp)


def folding(hy):
    j = lax.broadcasted_iota(jnp.int32, (1, QUAD), 1)
    lanes = lax.broadcasted_iota(jnp.int32, (QUAD, QUAD), 0)
    return jnp.where(lanes == fold_lane(j, hy), 1.0, 0.0).astype(jnp.bfloat16)


def unfolding(hy):
    j = lax.broadcasted_iota(jnp.int32, (QUAD, 1), 0)
    lanes = lax.broadcasted_iota(jnp.int32, (QUAD, QUAD), 1)
    return jnp.where(lanes == fold_lane(j, hy), 1.0, 0.0).astype(jnp.bfloat16)


def chunk_home(n):
    hy = n // 2
    h = n if hy == 0 else 3 - n
    return [slice((hy * 2 + hz) * QUAD + h * 128, (hy * 2 + hz) * QUAD + h * 128 + 128) for hz in (0, 1)]


def butterfly(v):
    q = [v[:, i * QUAD : (i + 1) * QUAD] for i in range(4)]
    sy0, sy1, dy0, dy1 = q[0] + q[2], q[1] + q[3], q[0] - q[2], q[1] - q[3]
    return jnp.concatenate([sy0 + sy1, sy0 - sy1, dy0 + dy1, dy0 - dy1], axis=1)


def split(v):
    hi = v.astype(jnp.bfloat16)
    lo = (v - hi.astype(jnp.float32)).astype(jnp.bfloat16)
    return hi, lo


def dot3(v, hi_mat, lo_mat):
    hi, lo = split(v)
    rows = v.shape[0]
    both = jnp.dot(
        jnp.concatenate([hi, lo], axis=0), hi_mat, preferred_element_type=jnp.float32
    )
    low = jnp.dot(hi, lo_mat, preferred_element_type=jnp.float32)
    return both[:rows] + both[rows:] + low


GROUP = 16


def prep_kernel(orb_ref, pot_ref, own_ref, planes_ref, fold):
    @pl.when(pl.program_id(0) == 0)
    def _():
        fold[0] = folding(0)
        fold[1] = folding(1)
        rest = pot_ref[...]
        planes = []
        for _ in range(3):
            top = rest.astype(jnp.bfloat16).astype(jnp.float32)
            planes.append(top)
            rest = rest - top
        x = jnp.concatenate(planes + [jnp.zeros_like(rest)], axis=0).astype(jnp.bfloat16)
        for n in range(4):
            y = jnp.dot(
                x[:, n * QUAD : (n + 1) * QUAD], fold[n // 2], preferred_element_type=jnp.float32
            )
            for hz, lanes in enumerate(chunk_home(n)):
                for p in range(4):
                    part = y[p * CX : (p + 1) * CX, hz * 128 : hz * 128 + 128]
                    planes_ref[p // 2, p % 2, :, lanes] = part.astype(jnp.bfloat16)

    x = orb_ref[...].astype(jnp.float32)
    x = x.reshape(GROUP * CX, CROSS).astype(jnp.bfloat16)
    for n in range(4):
        y = jnp.dot(
            x[:, n * QUAD : (n + 1) * QUAD], fold[n // 2], preferred_element_type=jnp.float32
        )
        for hz, lanes in enumerate(chunk_home(n)):
            part = y[:, hz * 128 : hz * 128 + 128].reshape(GROUP, CX, 128)
            own_ref[:, :, lanes] = part.astype(jnp.bfloat16)


def solve_kernel(
    idx_ref, shift_ref, partner_ref, member_ref,
    own_hbm, win_hbm, pot_ref, potw_ref,
    ktab_hbm, ltab_hbm, inv_ref, a3_ref, b3_ref, lx_ref,
    out_ref, table_ref,
    own_ref, win_ref, ktab_ref, ltab_ref, ktr_ref,
    wv, pots, acc, stg, home, listed, sems,
):
    slab = idx_ref[0]
    core = idx_ref[1]
    loads = [
        pltpu.make_async_copy(own_hbm, own_ref, sems.at[0]),
        *(
            pltpu.make_async_copy(win_hbm.at[k], win_ref.at[k], sems.at[1 + k])
            for k in range(WIDTH)
        ),
        pltpu.make_async_copy(ltab_hbm, ltab_ref, sems.at[WIDTH + 1]),
        pltpu.make_async_copy(ktab_hbm, ktab_ref, sems.at[WIDTH + 2]),
    ]
    for load in loads:
        load.start()

    def rank_colour(c, ranks):
        cl = shift_ref[c] >> 3
        a = sum(jnp.where(cl == n, rank, 0) for n, rank in enumerate(ranks))
        k = (slab - cl) & 3
        near = jnp.where(k == 0, 1, 0)
        box = (a & 1) * MINE + (a >> 1)
        t = ((k + 3) & 3) * 2 * MINE
        table_ref[c] = t + box + (box << 7) + (near << 12)
        home[jnp.where(k == 0, a, 31)] = c
        return tuple(rank + jnp.where(cl == n, 1, 0) for n, rank in enumerate(ranks))

    lax.fori_loop(0, NCOL, rank_colour, (jnp.int32(0),) * WIDTH, unroll=4)
    base = 256 - slab * CX

    count = jnp.int32(0)
    for t in range(3):
        block = slab * 3 + t

        def list_slot(p, count, t=t, block=block):
            pid = partner_ref[p, block]
            a = t * MEMBERS + member_ref[p, block]
            live = jnp.logical_and(pid >= 0, (a & 1) == core)
            pid = jnp.maximum(pid, 0)
            cj = pid >> 4
            rel = (((pid & 15) << 5) + shift_ref[cj] + base) & 511
            listed[count] = ((rel - 224) << 19) + (cj << 12) + (home[a] << 5) + a
            return count + jnp.where(live, 1, 0)

        count = lax.fori_loop(0, SLOTS // 3, list_slot, count, unroll=8)
    for extra in range(BATCH):
        listed[count + extra] = 1024 << 19

    def pair(n):
        word = listed[n]
        ci = (word >> 5) & 127
        return (word >> 1) & 15, ci, (word >> 12) & 127, shift_ref[ci] & 7, (word >> 19) - 32

    lead = idx_ref[2] * WIDTH * CX
    lead_rows = pl.ds(pl.multiple_of(lead, CX), CX)
    tail_rows = pl.ds(pl.multiple_of(WIDTH * CX - lead, CX), CX)

    def whole(planes):
        f = jnp.float32
        return planes[0, 0].astype(f) + planes[0, 1].astype(f) + planes[1, 0].astype(f)

    pots[lead_rows] = whole(pot_ref)
    pots[tail_rows] = whole(potw_ref.at[WIDTH - 1])
    for k in range(1, WIDTH):
        pots[k * CX : (k + 1) * CX] = whole(potw_ref.at[k - 1])

    def widen(rows, source):
        def one(c, _):
            wv[c, rows] = source[c].astype(jnp.float32)
            return 0

        lax.fori_loop(0, NCOL, one, 0, unroll=4)

    loads[0].wait()
    widen(lead_rows, own_ref)
    for k in range(WIDTH):
        loads[1 + k].wait()
        rows = tail_rows if k == WIDTH - 1 else slice((k + 1) * CX, (k + 2) * CX)
        widen(rows, win_ref.at[k])
    loads[WIDTH + 1].wait()
    loads[WIDTH + 2].wait()
    for h in range(2):
        for q in range(4):
            ktr_ref[h, q] = ktab_ref[h, q].astype(jnp.float32).T.astype(jnp.bfloat16)

    row_ids = lax.broadcasted_iota(jnp.int32, (WIN, 1), 0)

    for group in range(2):
        for j in range(6):
            i = group * 6 + j
            c = home[2 * i + core]
            sub = shift_ref[c] % CX
            inside = jnp.logical_and(row_ids >= sub, row_ids < sub + B)
            w = jnp.where(inside, wv[c], 0.0)
            stg[j * WIN : (j + 1) * WIN] = butterfly(w)
            twice = jnp.concatenate([w, w], axis=0).astype(jnp.bfloat16)
            acc[i] = pots[...] * w + jnp.dot(
                lx_ref[sub][:, :80], twice, preferred_element_type=jnp.float32
            )
        for q in range(4):
            cols = slice(q * QUAD, (q + 1) * QUAD)
            v = stg[0 : 6 * WIN, cols]
            stg[0 : 6 * WIN, cols] = dot3(v, ltab_ref[0, q], ltab_ref[1, q])
        for j in range(6):
            i = group * 6 + j
            acc[i] = acc[i] + butterfly(stg[j * WIN : (j + 1) * WIN])

    lane_ids = lax.broadcasted_iota(jnp.int32, (1, 128), 1)
    lane_row = lane_ids - WIN * jnp.where(lane_ids >= WIN, 1, 0)
    lane_row = lane_row - WIN * jnp.where(lane_ids >= 2 * WIN, 1, 0)

    def batch(b, _):
        for p in range(BATCH):
            _, ci, cj, sub, lo = pair(b * BATCH + p)
            held = jnp.logical_and(lane_row >= lo, lane_row < lo + B)
            left = jnp.where(held, a3_ref[sub], 0.0).astype(jnp.bfloat16)
            dens = wv[ci] * wv[cj]
            hi = dens.astype(jnp.bfloat16).astype(jnp.float32)
            stack = jnp.concatenate(
                [hi, dens - hi, hi, jnp.zeros((CX, CROSS), jnp.float32)], axis=0
            ).astype(jnp.bfloat16)
            u = jnp.dot(left, stack, preferred_element_type=jnp.float32)
            stg[p * B : (p + 1) * B] = butterfly(u)
        for q in range(4):
            cols = slice(q * QUAD, (q + 1) * QUAD)
            g = dot3(stg[:, cols], ktab_ref[0, q], ktab_ref[1, q])
            g = g.reshape(BATCH, B, QUAD) * inv_ref[:, cols][None]
            g = g.reshape(BATCH * B, QUAD)
            stg[:, cols] = dot3(g, ktr_ref[0, q], ktr_ref[1, q])
        for p in range(BATCH):
            m, _, cj, sub, lo = pair(b * BATCH + p)
            held = jnp.logical_and(row_ids >= lo, row_ids < lo + B)
            right = jnp.where(held, b3_ref[sub], 0.0).astype(jnp.bfloat16)
            hi, low = split(butterfly(stg[p * B : (p + 1) * B]))
            stack = jnp.concatenate([hi, low, hi], axis=0)
            field = jnp.dot(right[:, :96], stack, preferred_element_type=jnp.float32)
            acc[m] = acc[m] + field * wv[cj]
        return 0

    lax.fori_loop(0, (count + BATCH - 1) // BATCH, batch, 0)

    for n in range(4):
        back = unfolding(n // 2)
        low_z, high_z = chunk_home(n)
        for group in range(2):
            rows = slice(group * 6, group * 6 + 6)
            v = jnp.concatenate([acc[rows, :, low_z], acc[rows, :, high_z]], axis=2)
            hi, lo = split(v.reshape(6 * WIN, QUAD))
            y = jnp.dot(
                jnp.concatenate([hi, lo], axis=0), back, preferred_element_type=jnp.float32
            )
            y = y[: 6 * WIN] + y[6 * WIN :]
            for j in range(6):
                for k in range(WIDTH + 1):
                    first = j * WIN + k * CX
                    out_ref[k, group * 6 + j, :, n * QUAD : (n + 1) * QUAD] = y[
                        first : first + CX
                    ]


def slab_at(step):
    s = lax.axis_index("orb")
    group = lax.axis_index("group")
    y, zl, zh, core = s % 4, (s // 4) % 4, group // 2, group % 2
    if step > 0:
        turn = (zl + (y + step) // 4) // 4
    else:
        turn = 1 - (zl - (1 - (y + step + 4) // 4) + 4) // 4
    return ((zh + turn) % 2 * 2 + core, (s + step + SLABS) % SLABS)


def ring(step):
    s = lax.axis_index("orb")
    return (lax.axis_index("group"), s - s % 4 + (s % 4 + step + 4) % 4)


def either(which, first, second):
    return tuple(a + which * (b - a) for a, b in zip(first, second))


def sibling():
    group = lax.axis_index("group")
    return (group // 2 * 2 + 1 - group % 2, lax.axis_index("orb"))


def greet(others):
    barrier = pltpu.get_barrier_semaphore()
    for other in others:
        pl.semaphore_signal(
            barrier, inc=1, device_id=other, device_id_type=pl.DeviceIdType.MESH
        )
    pl.semaphore_wait(barrier, len(others))


def remote(src, dst, send, recv, device):
    return pltpu.make_async_remote_copy(
        src_ref=src,
        dst_ref=dst,
        send_sem=send,
        recv_sem=recv,
        device_id=device,
        device_id_type=pl.DeviceIdType.MESH,
    )


def fetch_kernel(own, pot, win, potw, send, recv, dsend, drecv):
    core = lax.axis_index("group") % 2
    y = lax.axis_index("orb") % 4
    high, odd = y // 2, y % 2
    greet([ring(-1), ring(1), slab_at(-4), slab_at(4), sibling()])

    def mine(q):
        return pot.at[core] if q == PIECES else own.at[pl.ds(core * HALF + q * PIECE, PIECE)]

    def held(t, q):
        if q == PIECES:
            return potw.at[t, core]
        return win.at[t, pl.ds(core * HALF + q * PIECE, PIECE)]

    def move(stream, src, t, q, device):
        return remote(src, held(t, q), send.at[stream, q], recv.at[t, q], device)

    def to_sibling(t, q):
        return remote(held(t, q), held(t, q), dsend.at[t, q], drecv.at[t, q], sibling())

    relayed = 2 - 2 * odd
    onward = either(odd, ring(1), ring(-1))
    copies = {
        0: (None, lambda q: move(0, mine(q), 3, q, either(high, slab_at(-4), slab_at(4)))),
        1: (y != 3, lambda q: move(1, mine(q), 0, q, ring(-1))),
        2: (y == 3, lambda q: move(1, held(3, q), 0, q, ring(-1))),
        3: (y != 0, lambda q: move(2, mine(q), 2, q, ring(1))),
        4: (y == 0, lambda q: move(2, held(3, q), 2, q, ring(1))),
        5: (None, lambda q: move(3, held(relayed, q), 1, q, onward)),
    }

    def act(which, q, what):
        cond, make = copies[which]
        if cond is None:
            getattr(make(q), what)()
        else:

            @pl.when(cond)
            def _():
                getattr(make(q), what)()

    def arrived(t, q):
        move(0, held(t, q), t, q, sibling()).wait_recv()
        to_sibling(t, q).start()

    turns = range(PIECES + 1)
    for q in turns:
        for which in (0, 1, 3):
            act(which, q, "start")
    for q in turns:
        arrived(3, q)
        act(2, q, "start")
        act(4, q, "start")
        arrived(relayed, q)
        act(5, q, "start")
    for q in turns:
        arrived(2 - relayed, q)
    for q in turns:
        arrived(1, q)
    for q in turns:
        for which in range(6):
            act(which, q, "wait_send")
        for t in range(WIDTH):
            to_sibling(t, q).wait()


def spread_kernel(
    table_ref, boxes, out, got, ext, stage,
    send, recv, rsend, rrecv, dsend, drecv, osend, orecv, ksem,
):
    core = lax.axis_index("group") % 2
    slab = lax.axis_index("orb")
    y = slab % 4
    high, odd = y // 2, y % 2
    greet(
        [ring(-1), ring(1), slab_at(-4), slab_at(4), slab_at(-3), slab_at(3), sibling()]
    )

    def part(q):
        return pl.ds(q * BOXES, BOXES)

    def landing(t, q):
        return got.at[pl.ds((t * 2 + core) * MINE + q * BOXES, BOXES)]

    def ship(t, src, q, device):
        return remote(src, landing(t, q), send.at[t, q], recv.at[t, q], device)

    low_cross = (y % 2) * (1 - high)
    high_cross = (1 - y % 2) * high
    to_one = either(high_cross, ring(1), slab_at(-3))
    to_three = either(low_cross, ring(-1), slab_at(3))
    to_z = either(high, slab_at(4), slab_at(-4))
    outer = WIDTH * (1 - high)
    inner = WIDTH * high

    def by_z(q):
        return ship(3, boxes.at[outer, part(q)], q, to_z)

    def by_one(q):
        return ship(0, boxes.at[1, part(q)], q, to_one)

    def by_three(q):
        return ship(2, boxes.at[3, part(q)], q, to_three)

    def to_relay(q):
        return remote(
            boxes.at[2, part(q)],
            stage.at[part(q)],
            rsend.at[q],
            rrecv.at[q],
            either(odd, ring(1), ring(-1)),
        )

    def relay(q):
        return ship(1, stage.at[part(q)], q, either(odd, ring(-1), ring(1)))

    def to_sibling(t, q):
        here = landing(t, q)
        return remote(here, here, dsend.at[t, q], drecv.at[t, q], sibling())

    def arrived(t, q):
        ship(t, boxes.at[0, part(q)], q, sibling()).wait_recv()
        to_sibling(t, q).start()

    local = remote(boxes.at[inner], ext.at[pl.ds(core * MINE, MINE)], osend, orecv, sibling())
    for q in range(SHIPS):
        to_relay(q).start()
    for q in range(SHIPS):
        by_z(q).start()
        by_one(q).start()
        by_three(q).start()
    local.start()
    keep = pltpu.make_async_copy(boxes.at[inner], ext.at[pl.ds(core * MINE, MINE)], ksem)
    keep.start()
    for q in range(SHIPS):
        to_relay(q).wait_recv()
        relay(q).start()
    for q in range(SHIPS):
        arrived(3, q)
        arrived(0, q)
        arrived(2, q)
    for q in range(SHIPS):
        arrived(1, q)
    local.wait()
    keep.wait()
    for q in range(SHIPS):
        to_relay(q).wait_send()
        for copy in (by_z(q), by_one(q), by_three(q), relay(q)):
            copy.wait_send()
        for t in range(WIDTH):
            to_sibling(t, q).wait()

    def place(c, _):
        word = table_ref[c]
        extra = jnp.where((word >> 12) == 1, 1.0, 0.0)
        out[c] = got[word & 127] + extra * ext[(word >> 7) & 31]
        return 0

    lax.fori_loop(0, NCOL, place, 0, unroll=8)


def body(orbitals, potential, box_shift, pair_partner, pair_member):
    ktab, ltab, inv, a3, b3, lx = tables()
    place = lax.axis_index("orb").astype(jnp.int32)
    high = place % 4 // 2
    slab = (place - 4 * high) % SLABS
    core = lax.axis_index("group").astype(jnp.int32) % 2
    smem = pl.BlockSpec(memory_space=pltpu.SMEM)
    vmem = pl.BlockSpec(memory_space=pltpu.VMEM)
    hbm = pl.BlockSpec(memory_space=pltpu.HBM)
    dma = pltpu.SemaphoreType.DMA
    own, pot = pl.pallas_call(
        prep_kernel,
        out_shape=(
            jax.ShapeDtypeStruct((NCOL, CX, CROSS), jnp.bfloat16),
            jax.ShapeDtypeStruct((2, 2, CX, CROSS), jnp.bfloat16),
        ),
        grid=(NCOL // GROUP,),
        in_specs=[
            pl.BlockSpec((GROUP, CX, CROSS), lambda g: (g, 0, 0)),
            pl.BlockSpec((CX, CROSS), lambda g: (0, 0)),
        ],
        out_specs=(
            pl.BlockSpec((GROUP, CX, CROSS), lambda g: (g, 0, 0)),
            pl.BlockSpec((2, 2, CX, CROSS), lambda g: (0, 0, 0, 0)),
        ),
        scratch_shapes=[pltpu.VMEM((2, QUAD, QUAD), jnp.bfloat16)],
        name="prep",
    )(orbitals, potential)
    streams = (WIDTH, PIECES + 1)
    win, potw = pl.pallas_call(
        fetch_kernel,
        out_shape=(
            jax.ShapeDtypeStruct((WIDTH, NCOL, CX, CROSS), jnp.bfloat16),
            jax.ShapeDtypeStruct((WIDTH, 2, 2, CX, CROSS), jnp.bfloat16),
        ),
        in_specs=[hbm] * 2,
        out_specs=(hbm, hbm),
        scratch_shapes=[dma(streams)] * 4,
        compiler_params=pltpu.CompilerParams(collective_id=0, has_side_effects=True),
        name="fetch",
    )(own, pot)
    idx = jnp.stack([slab, core, high])
    boxes, table = pl.pallas_call(
        solve_kernel,
        out_shape=(
            jax.ShapeDtypeStruct((WIDTH + 1, MINE, CX, CROSS), jnp.float32),
            jax.ShapeDtypeStruct((NCOL,), jnp.int32),
        ),
        in_specs=[smem] * 4 + [hbm] * 2 + [vmem] * 2 + [hbm] * 2 + [vmem] * 4,
        out_specs=(vmem, smem),
        scratch_shapes=[
            pltpu.VMEM((NCOL, CX, CROSS), jnp.bfloat16),
            pltpu.VMEM((WIDTH, NCOL, CX, CROSS), jnp.bfloat16),
        ]
        + [pltpu.VMEM((2, 4, QUAD, QUAD), jnp.bfloat16)] * 3
        + [
            pltpu.VMEM((NCOL, WIN, CROSS), jnp.float32),
            pltpu.VMEM((WIN, CROSS), jnp.float32),
            pltpu.VMEM((MINE, WIN, CROSS), jnp.float32),
            pltpu.VMEM((BATCH * B, CROSS), jnp.float32),
            pltpu.SMEM((32,), jnp.int32),
        ]
        + [pltpu.SMEM((SLOTS + BATCH,), jnp.int32)]
        + [dma((WIDTH + 3,))],
        compiler_params=pltpu.CompilerParams(vmem_limit_bytes=44 * 2**20),
        name="solve",
    )(idx, box_shift, pair_partner.T, pair_member.T, own, win, pot, potw, ktab, ltab, inv, a3, b3, lx)
    piece = (MINE, CX, CROSS)
    ships = (WIDTH, SHIPS)
    return pl.pallas_call(
        spread_kernel,
        out_shape=jax.ShapeDtypeStruct((NCOL, CX, CROSS), jnp.float32),
        in_specs=[smem, hbm],
        out_specs=vmem,
        scratch_shapes=[
            pltpu.VMEM((WIDTH * 2 * MINE, CX, CROSS), jnp.float32),
            pltpu.VMEM((2 * MINE, CX, CROSS), jnp.float32),
            pltpu.VMEM(piece, jnp.float32),
            dma(ships),
            dma(ships),
            dma((SHIPS,)),
            dma((SHIPS,)),
            dma(ships),
            dma(ships),
            dma,
            dma,
            dma,
        ],
        compiler_params=pltpu.CompilerParams(
            collective_id=1, has_side_effects=True, vmem_limit_bytes=40 * 2**20
        ),
        name="spread",
    )(table, boxes)


def solution(mesh):
    placed = (P(None, "orb", None), P("orb", None), P(), P(), P())
    return jax.shard_map(
        body, mesh=mesh, in_specs=placed, out_specs=P(None, "orb", None), check_vma=False
    )
```

```python
import functools

import jax
import jax.numpy as jnp
import numpy as np
from jax import lax
from jax.experimental import pallas as pl
from jax.experimental.pallas import tpu as pltpu
from jax.sharding import PartitionSpec as P

B = 32
CX = 8
MEMBERS = 8
NCOL = 96
HALF = NCOL // 2
SLABS = 64
WIDTH = 4
CROSS = B * B
QUAD = CROSS // 4
WIN = (WIDTH + 1) * CX
MINE = 12
BATCH = 8
SLOTS = 168
PIECES = 8
PIECE = HALF // PIECES
SHIPS = 4
BOXES = MINE // SHIPS

lap_weights = (
    -5369.0 / 1800.0,
    12.0 / 7.0,
    -15.0 / 56.0,
    10.0 / 189.0,
    -1.0 / 112.0,
    2.0 / 1925.0,
    -1.0 / 16632.0,
)
stencil_reach = 6
mixing = 0.25


def halves(values):
    hi = values.astype(jnp.bfloat16).astype(np.float64)
    lo = (values - hi).astype(jnp.bfloat16).astype(np.float64)
    return hi, lo


def tables():
    idx = np.arange(1, B + 1)
    sine = np.sqrt(2.0 / (B + 1)) * np.sin(np.pi * np.outer(idx, idx) / (B + 1))
    single = 2.0 - 2.0 * np.cos(np.pi * idx / (B + 1))
    part = [sine[: B // 2, p::2] for p in (0, 1)]
    lap = np.zeros((B, B))
    for o, w in enumerate(lap_weights):
        lap += w * (np.eye(B, k=o) if o == 0 else np.eye(B, k=o) + np.eye(B, k=-o))
    flip = lap[: B // 2, ::-1][:, : B // 2]
    fold = [lap[: B // 2, : B // 2] + flip, lap[: B // 2, : B // 2] - flip]
    eye = np.eye(B // 2)
    kmat, lmat, modes = [], [], []
    for py in (0, 1):
        for pz in (0, 1):
            kmat.append(np.kron(part[py], part[pz]))
            lmat.append(-0.125 * (np.kron(fold[py], eye) + np.kron(eye, fold[pz])).T)
            cross = single[py::2][:, None] + single[pz::2][None, :]
            modes.append(single[:, None] + cross.reshape(1, -1))
    inv = (-mixing / np.concatenate(modes, axis=1)).astype(np.float32)
    ktab = np.stack(halves(np.stack(kmat))).astype(jnp.bfloat16)
    ltab = np.stack(halves(np.stack(lmat))).astype(jnp.bfloat16)
    a3 = np.zeros((CX, B, 128))
    b3 = np.zeros((CX, WIN, 128))
    lx = np.zeros((CX, WIN, 128))
    for sub in range(CX):
        placed = np.zeros((B, WIN))
        placed[:, sub : sub + B] = sine
        hi, lo = halves(placed)
        a3[sub, :, :120] = np.concatenate([hi, hi, lo], axis=1)
        b3[sub, :, :96] = np.concatenate([hi.T, hi.T, lo.T], axis=1)
        lap_placed = np.zeros((WIN, WIN))
        lap_placed[sub : sub + B, sub : sub + B] = -0.5 * lap
        hi, lo = halves(lap_placed)
        lx[sub, :, :80] = np.concatenate([hi, lo], axis=1)
    return (
        ktab,
        ltab,
        inv,
        a3.astype(np.float32),
        b3.astype(np.float32),
        lx.astype(jnp.bfloat16),
    )


def fold_lane(j, hy):
    hz, yp, zp = j // 128, j % 128 // 16, j % 16
    yl = yp if hy == 0 else 7 - yp
    return yl * B + zp + hz * (B - 1 - 2 * zp)


def folding(hy):
    j = lax.broadcasted_iota(jnp.int32, (1, QUAD), 1)
    lanes = lax.broadcasted_iota(jnp.int32, (QUAD, QUAD), 0)
    return jnp.where(lanes == fold_lane(j, hy), 1.0, 0.0).astype(jnp.bfloat16)


def unfolding(hy):
    j = lax.broadcasted_iota(jnp.int32, (QUAD, 1), 0)
    lanes = lax.broadcasted_iota(jnp.int32, (QUAD, QUAD), 1)
    return jnp.where(lanes == fold_lane(j, hy), 1.0, 0.0).astype(jnp.bfloat16)


def chunk_home(n):
    hy = n // 2
    h = n if hy == 0 else 3 - n
    return [slice((hy * 2 + hz) * QUAD + h * 128, (hy * 2 + hz) * QUAD + h * 128 + 128) for hz in (0, 1)]


def butterfly(v):
    q = [v[:, i * QUAD : (i + 1) * QUAD] for i in range(4)]
    sy0, sy1, dy0, dy1 = q[0] + q[2], q[1] + q[3], q[0] - q[2], q[1] - q[3]
    return jnp.concatenate([sy0 + sy1, sy0 - sy1, dy0 + dy1, dy0 - dy1], axis=1)


def split(v):
    hi = v.astype(jnp.bfloat16)
    lo = (v - hi.astype(jnp.float32)).astype(jnp.bfloat16)
    return hi, lo


def dot3(v, hi_mat, lo_mat):
    hi, lo = split(v)
    rows = v.shape[0]
    both = jnp.dot(
        jnp.concatenate([hi, lo], axis=0), hi_mat, preferred_element_type=jnp.float32
    )
    low = jnp.dot(hi, lo_mat, preferred_element_type=jnp.float32)
    return both[:rows] + both[rows:] + low


GROUP = 32


def prep_kernel(orb_ref, pot_ref, own_ref, planes_ref):
    fold = [folding(0), folding(1)]

    def some(g, _):
        x = orb_ref[pl.ds(g * GROUP, GROUP)].astype(jnp.float32)
        x = x.reshape(GROUP * CX, CROSS).astype(jnp.bfloat16)
        for n in range(4):
            y = jnp.dot(
                x[:, n * QUAD : (n + 1) * QUAD],
                fold[n // 2],
                preferred_element_type=jnp.float32,
            )
            for hz, lanes in enumerate(chunk_home(n)):
                part = y[:, hz * 128 : hz * 128 + 128].reshape(GROUP, CX, 128)
                own_ref[pl.ds(g * GROUP, GROUP), :, lanes] = part.astype(jnp.bfloat16)
        return 0

    lax.fori_loop(0, NCOL // GROUP, some, 0)
    rest = pot_ref[...]
    planes = []
    for _ in range(3):
        top = rest.astype(jnp.bfloat16).astype(jnp.float32)
        planes.append(top)
        rest = rest - top
    x = jnp.concatenate(planes + [jnp.zeros_like(rest)], axis=0).astype(jnp.bfloat16)
    for n in range(4):
        y = jnp.dot(
            x[:, n * QUAD : (n + 1) * QUAD], fold[n // 2], preferred_element_type=jnp.float32
        )
        for hz, lanes in enumerate(chunk_home(n)):
            for p in range(4):
                part = y[p * CX : (p + 1) * CX, hz * 128 : hz * 128 + 128]
                planes_ref[p // 2, p % 2, :, lanes] = part.astype(jnp.bfloat16)


def solve_kernel(
    idx_ref, shift_ref, partner_ref, member_ref,
    own_hbm, win_hbm, pot_hbm, potw_hbm,
    ktab_hbm, ltab_hbm, inv_ref, a3_ref, b3_ref, lx_ref,
    out_ref, table_ref,
    own_ref, win_ref, pot_ref, potw_ref, ktab_ref, ltab_ref, ktr_ref,
    wv, pots, acc, stg, home, listed, sems,
):
    slab = idx_ref[0]
    core = idx_ref[1]
    loads = [
        pltpu.make_async_copy(own_hbm, own_ref, sems.at[0]),
        *(
            pltpu.make_async_copy(win_hbm.at[k], win_ref.at[k], sems.at[1 + k])
            for k in range(WIDTH)
        ),
        pltpu.make_async_copy(ltab_hbm, ltab_ref, sems.at[WIDTH + 1]),
        pltpu.make_async_copy(ktab_hbm, ktab_ref, sems.at[WIDTH + 2]),
        pltpu.make_async_copy(pot_hbm, pot_ref, sems.at[WIDTH + 3]),
        pltpu.make_async_copy(potw_hbm, potw_ref, sems.at[WIDTH + 4]),
    ]
    for load in loads:
        load.start()

    def rank_colour(c, ranks):
        cl = shift_ref[c] >> 3
        a = sum(jnp.where(cl == n, rank, 0) for n, rank in enumerate(ranks))
        k = (slab - cl) & 3
        near = jnp.where(k == 0, 1, 0)
        box = (a & 1) * MINE + (a >> 1)
        t = ((k + 3) & 3) * 2 * MINE
        table_ref[c] = t + box + (box << 7) + (near << 12)
        home[jnp.where(k == 0, a, 31)] = c
        return tuple(rank + jnp.where(cl == n, 1, 0) for n, rank in enumerate(ranks))

    lax.fori_loop(0, NCOL, rank_colour, (jnp.int32(0),) * WIDTH, unroll=4)
    base = 256 - slab * CX

    count = jnp.int32(0)
    for t in range(3):
        block = slab * 3 + t

        def list_slot(p, count, t=t, block=block):
            pid = partner_ref[p, block]
            a = t * MEMBERS + member_ref[p, block]
            live = jnp.logical_and(pid >= 0, (a & 1) == core)
            pid = jnp.maximum(pid, 0)
            cj = pid >> 4
            rel = (((pid & 15) << 5) + shift_ref[cj] + base) & 511
            listed[count] = ((rel - 224) << 19) + (cj << 12) + (home[a] << 5) + a
            return count + jnp.where(live, 1, 0)

        count = lax.fori_loop(0, SLOTS // 3, list_slot, count, unroll=8)
    for extra in range(BATCH):
        listed[count + extra] = 1024 << 19

    def pair(n):
        word = listed[n]
        ci = (word >> 5) & 127
        return (word >> 1) & 15, ci, (word >> 12) & 127, shift_ref[ci] & 7, (word >> 19) - 32

    lead = idx_ref[2] * WIDTH * CX
    lead_rows = pl.ds(pl.multiple_of(lead, CX), CX)
    tail_rows = pl.ds(pl.multiple_of(WIDTH * CX - lead, CX), CX)

    def whole(planes):
        f = jnp.float32
        return planes[0, 0].astype(f) + planes[0, 1].astype(f) + planes[1, 0].astype(f)

    def widen(rows, source):
        def one(c, _):
            wv[c, rows] = source[c].astype(jnp.float32)
            return 0

        lax.fori_loop(0, NCOL, one, 0, unroll=4)

    loads[0].wait()
    widen(lead_rows, own_ref)
    for k in range(WIDTH):
        loads[1 + k].wait()
        rows = tail_rows if k == WIDTH - 1 else slice((k + 1) * CX, (k + 2) * CX)
        widen(rows, win_ref.at[k])
    loads[WIDTH + 1].wait()
    loads[WIDTH + 2].wait()
    loads[WIDTH + 3].wait()
    loads[WIDTH + 4].wait()
    pots[lead_rows] = whole(pot_ref)
    pots[tail_rows] = whole(potw_ref.at[WIDTH - 1])
    for k in range(1, WIDTH):
        pots[k * CX : (k + 1) * CX] = whole(potw_ref.at[k - 1])
    for h in range(2):
        for q in range(4):
            ktr_ref[h, q] = ktab_ref[h, q].astype(jnp.float32).T.astype(jnp.bfloat16)

    row_ids = lax.broadcasted_iota(jnp.int32, (WIN, 1), 0)

    for group in range(2):
        for j in range(6):
            i = group * 6 + j
            c = home[2 * i + core]
            sub = shift_ref[c] % CX
            inside = jnp.logical_and(row_ids >= sub, row_ids < sub + B)
            w = jnp.where(inside, wv[c], 0.0)
            stg[j * WIN : (j + 1) * WIN] = butterfly(w)
            twice = jnp.concatenate([w, w], axis=0).astype(jnp.bfloat16)
            acc[i] = pots[...] * w + jnp.dot(
                lx_ref[sub][:, :80], twice, preferred_element_type=jnp.float32
            )
        for q in range(4):
            cols = slice(q * QUAD, (q + 1) * QUAD)
            v = stg[0 : 6 * WIN, cols]
            stg[0 : 6 * WIN, cols] = dot3(v, ltab_ref[0, q], ltab_ref[1, q])
        for j in range(6):
            i = group * 6 + j
            acc[i] = acc[i] + butterfly(stg[j * WIN : (j + 1) * WIN])

    lane_ids = lax.broadcasted_iota(jnp.int32, (1, 128), 1)
    lane_row = lane_ids - WIN * jnp.where(lane_ids >= WIN, 1, 0)
    lane_row = lane_row - WIN * jnp.where(lane_ids >= 2 * WIN, 1, 0)

    def batch(b, _):
        for p in range(BATCH):
            _, ci, cj, sub, lo = pair(b * BATCH + p)
            held = jnp.logical_and(lane_row >= lo, lane_row < lo + B)
            left = jnp.where(held, a3_ref[sub], 0.0).astype(jnp.bfloat16)
            dens = wv[ci] * wv[cj]
            hi = dens.astype(jnp.bfloat16).astype(jnp.float32)
            stack = jnp.concatenate(
                [hi, dens - hi, hi, jnp.zeros((CX, CROSS), jnp.float32)], axis=0
            ).astype(jnp.bfloat16)
            u = jnp.dot(left, stack, preferred_element_type=jnp.float32)
            stg[p * B : (p + 1) * B] = butterfly(u)
        for q in range(4):
            cols = slice(q * QUAD, (q + 1) * QUAD)
            g = dot3(stg[:, cols], ktab_ref[0, q], ktab_ref[1, q])
            g = g.reshape(BATCH, B, QUAD) * inv_ref[:, cols][None]
            g = g.reshape(BATCH * B, QUAD)
            stg[:, cols] = dot3(g, ktr_ref[0, q], ktr_ref[1, q])
        for p in range(BATCH):
            m, _, cj, sub, lo = pair(b * BATCH + p)
            held = jnp.logical_and(row_ids >= lo, row_ids < lo + B)
            right = jnp.where(held, b3_ref[sub], 0.0).astype(jnp.bfloat16)
            hi, low = split(butterfly(stg[p * B : (p + 1) * B]))
            stack = jnp.concatenate([hi, low, hi], axis=0)
            field = jnp.dot(right[:, :96], stack, preferred_element_type=jnp.float32)
            acc[m] = acc[m] + field * wv[cj]
        return 0

    lax.fori_loop(0, (count + BATCH - 1) // BATCH, batch, 0)

    for n in range(4):
        back = unfolding(n // 2)
        low_z, high_z = chunk_home(n)
        for group in range(2):
            rows = slice(group * 6, group * 6 + 6)
            v = jnp.concatenate([acc[rows, :, low_z], acc[rows, :, high_z]], axis=2)
            hi, lo = split(v.reshape(6 * WIN, QUAD))
            y = jnp.dot(
                jnp.concatenate([hi, lo], axis=0), back, preferred_element_type=jnp.float32
            )
            y = y[: 6 * WIN] + y[6 * WIN :]
            for j in range(6):
                for k in range(WIDTH + 1):
                    first = j * WIN + k * CX
                    out_ref[k, group * 6 + j, :, n * QUAD : (n + 1) * QUAD] = y[
                        first : first + CX
                    ]


def slab_at(step):
    s = lax.axis_index("orb")
    group = lax.axis_index("group")
    y, zl, zh, core = s % 4, (s // 4) % 4, group // 2, group % 2
    if step > 0:
        turn = (zl + (y + step) // 4) // 4
    else:
        turn = 1 - (zl - (1 - (y + step + 4) // 4) + 4) // 4
    return ((zh + turn) % 2 * 2 + core, (s + step + SLABS) % SLABS)


def ring(step):
    s = lax.axis_index("orb")
    return (lax.axis_index("group"), s - s % 4 + (s % 4 + step + 4) % 4)


def either(which, first, second):
    return tuple(a + which * (b - a) for a, b in zip(first, second))


def sibling():
    group = lax.axis_index("group")
    return (group // 2 * 2 + 1 - group % 2, lax.axis_index("orb"))


def greet(others):
    barrier = pltpu.get_barrier_semaphore()
    for other in others:
        pl.semaphore_signal(
            barrier, inc=1, device_id=other, device_id_type=pl.DeviceIdType.MESH
        )
    pl.semaphore_wait(barrier, len(others))


def remote(src, dst, send, recv, device):
    return pltpu.make_async_remote_copy(
        src_ref=src,
        dst_ref=dst,
        send_sem=send,
        recv_sem=recv,
        device_id=device,
        device_id_type=pl.DeviceIdType.MESH,
    )


def fetch_kernel(own, pot, win, potw, send, recv, dsend, drecv):
    core = lax.axis_index("group") % 2
    y = lax.axis_index("orb") % 4
    high, odd = y // 2, y % 2
    greet([ring(-1), ring(1), slab_at(-4), slab_at(4), sibling()])

    def mine(q):
        return pot.at[core] if q == PIECES else own.at[pl.ds(core * HALF + q * PIECE, PIECE)]

    def held(t, q):
        if q == PIECES:
            return potw.at[t, core]
        return win.at[t, pl.ds(core * HALF + q * PIECE, PIECE)]

    def move(stream, src, t, q, device):
        return remote(src, held(t, q), send.at[stream, q], recv.at[t, q], device)

    def to_sibling(t, q):
        return remote(held(t, q), held(t, q), dsend.at[t, q], drecv.at[t, q], sibling())

    relayed = 2 - 2 * odd
    onward = either(odd, ring(1), ring(-1))
    copies = {
        0: (None, lambda q: move(0, mine(q), 3, q, either(high, slab_at(-4), slab_at(4)))),
        1: (y != 3, lambda q: move(1, mine(q), 0, q, ring(-1))),
        2: (y == 3, lambda q: move(1, held(3, q), 0, q, ring(-1))),
        3: (y != 0, lambda q: move(2, mine(q), 2, q, ring(1))),
        4: (y == 0, lambda q: move(2, held(3, q), 2, q, ring(1))),
        5: (None, lambda q: move(3, held(relayed, q), 1, q, onward)),
    }

    def act(which, q, what):
        cond, make = copies[which]
        if cond is None:
            getattr(make(q), what)()
        else:

            @pl.when(cond)
            def _():
                getattr(make(q), what)()

    def arrived(t, q):
        move(0, held(t, q), t, q, sibling()).wait_recv()
        to_sibling(t, q).start()

    turns = range(PIECES + 1)
    for q in turns:
        for which in (0, 1, 3):
            act(which, q, "start")
    for q in turns:
        arrived(3, q)
        act(2, q, "start")
        act(4, q, "start")
        arrived(relayed, q)
        act(5, q, "start")
    for q in turns:
        arrived(2 - relayed, q)
    for q in turns:
        arrived(1, q)
    for q in turns:
        for which in range(6):
            act(which, q, "wait_send")
        for t in range(WIDTH):
            to_sibling(t, q).wait()


def spread_kernel(
    table_ref, boxes, out, got, ext, stage,
    send, recv, rsend, rrecv, dsend, drecv, osend, orecv, ksem,
):
    core = lax.axis_index("group") % 2
    slab = lax.axis_index("orb")
    y = slab % 4
    high, odd = y // 2, y % 2
    greet(
        [ring(-1), ring(1), slab_at(-4), slab_at(4), slab_at(-3), slab_at(3), sibling()]
    )

    def part(q):
        return pl.ds(q * BOXES, BOXES)

    def landing(t, q):
        return got.at[pl.ds((t * 2 + core) * MINE + q * BOXES, BOXES)]

    def ship(t, src, q, device):
        return remote(src, landing(t, q), send.at[t, q], recv.at[t, q], device)

    low_cross = (y % 2) * (1 - high)
    high_cross = (1 - y % 2) * high
    to_one = either(high_cross, ring(1), slab_at(-3))
    to_three = either(low_cross, ring(-1), slab_at(3))
    to_z = either(high, slab_at(4), slab_at(-4))
    outer = WIDTH * (1 - high)
    inner = WIDTH * high

    def by_z(q):
        return ship(3, boxes.at[outer, part(q)], q, to_z)

    def by_one(q):
        return ship(0, boxes.at[1, part(q)], q, to_one)

    def by_three(q):
        return ship(2, boxes.at[3, part(q)], q, to_three)

    def to_relay(q):
        return remote(
            boxes.at[2, part(q)],
            stage.at[part(q)],
            rsend.at[q],
            rrecv.at[q],
            either(odd, ring(1), ring(-1)),
        )

    def relay(q):
        return ship(1, stage.at[part(q)], q, either(odd, ring(-1), ring(1)))

    def to_sibling(t, q):
        here = landing(t, q)
        return remote(here, here, dsend.at[t, q], drecv.at[t, q], sibling())

    def arrived(t, q):
        ship(t, boxes.at[0, part(q)], q, sibling()).wait_recv()
        to_sibling(t, q).start()

    local = remote(boxes.at[inner], ext.at[pl.ds(core * MINE, MINE)], osend, orecv, sibling())
    for q in range(SHIPS):
        to_relay(q).start()
    for q in range(SHIPS):
        by_z(q).start()
        by_one(q).start()
        by_three(q).start()
    local.start()
    keep = pltpu.make_async_copy(boxes.at[inner], ext.at[pl.ds(core * MINE, MINE)], ksem)
    keep.start()
    for q in range(SHIPS):
        to_relay(q).wait_recv()
        relay(q).start()
    for q in range(SHIPS):
        arrived(3, q)
        arrived(0, q)
        arrived(2, q)
    for q in range(SHIPS):
        arrived(1, q)
    local.wait()
    keep.wait()
    for q in range(SHIPS):
        to_relay(q).wait_send()
        for copy in (by_z(q), by_one(q), by_three(q), relay(q)):
            copy.wait_send()
        for t in range(WIDTH):
            to_sibling(t, q).wait()

    def place(c, _):
        word = table_ref[c]
        extra = jnp.where((word >> 12) == 1, 1.0, 0.0)
        out[c] = got[word & 127] + extra * ext[(word >> 7) & 31]
        return 0

    lax.fori_loop(0, NCOL, place, 0, unroll=8)


def body(orbitals, potential, box_shift, pair_partner, pair_member):
    ktab, ltab, inv, a3, b3, lx = tables()
    place = lax.axis_index("orb").astype(jnp.int32)
    high = place % 4 // 2
    slab = (place - 4 * high) % SLABS
    core = lax.axis_index("group").astype(jnp.int32) % 2
    smem = pl.BlockSpec(memory_space=pltpu.SMEM)
    vmem = pl.BlockSpec(memory_space=pltpu.VMEM)
    hbm = pl.BlockSpec(memory_space=pltpu.HBM)
    dma = pltpu.SemaphoreType.DMA
    own, pot = pl.pallas_call(
        prep_kernel,
        out_shape=(
            jax.ShapeDtypeStruct((NCOL, CX, CROSS), jnp.bfloat16),
            jax.ShapeDtypeStruct((2, 2, CX, CROSS), jnp.bfloat16),
        ),
        in_specs=[vmem] * 2,
        out_specs=(vmem, vmem),
        compiler_params=pltpu.CompilerParams(vmem_limit_bytes=16 * 2**20),
        name="prep",
    )(orbitals, potential)
    streams = (WIDTH, PIECES + 1)
    win, potw = pl.pallas_call(
        fetch_kernel,
        out_shape=(
            jax.ShapeDtypeStruct((WIDTH, NCOL, CX, CROSS), jnp.bfloat16),
            jax.ShapeDtypeStruct((WIDTH, 2, 2, CX, CROSS), jnp.bfloat16),
        ),
        in_specs=[hbm] * 2,
        out_specs=(hbm, hbm),
        scratch_shapes=[dma(streams)] * 4,
        compiler_params=pltpu.CompilerParams(
            collective_id=0, has_side_effects=True, vmem_limit_bytes=2 * 2**20
        ),
        name="fetch",
    )(own, pot)
    idx = jnp.stack([slab, core, high])
    boxes, table = pl.pallas_call(
        solve_kernel,
        out_shape=(
            jax.ShapeDtypeStruct((WIDTH + 1, MINE, CX, CROSS), jnp.float32),
            jax.ShapeDtypeStruct((NCOL,), jnp.int32),
        ),
        in_specs=[smem] * 4 + [hbm] * 6 + [vmem] * 4,
        out_specs=(vmem, smem),
        scratch_shapes=[
            pltpu.VMEM((NCOL, CX, CROSS), jnp.bfloat16),
            pltpu.VMEM((WIDTH, NCOL, CX, CROSS), jnp.bfloat16),
            pltpu.VMEM((2, 2, CX, CROSS), jnp.bfloat16),
            pltpu.VMEM((WIDTH, 2, 2, CX, CROSS), jnp.bfloat16),
        ]
        + [pltpu.VMEM((2, 4, QUAD, QUAD), jnp.bfloat16)] * 3
        + [
            pltpu.VMEM((NCOL, WIN, CROSS), jnp.float32),
            pltpu.VMEM((WIN, CROSS), jnp.float32),
            pltpu.VMEM((MINE, WIN, CROSS), jnp.float32),
            pltpu.VMEM((BATCH * B, CROSS), jnp.float32),
            pltpu.SMEM((32,), jnp.int32),
        ]
        + [pltpu.SMEM((SLOTS + BATCH,), jnp.int32)]
        + [dma((WIDTH + 5,))],
        compiler_params=pltpu.CompilerParams(vmem_limit_bytes=40 * 2**20),
        name="solve",
    )(idx, box_shift, pair_partner.T, pair_member.T, own, win, pot, potw, ktab, ltab, inv, a3, b3, lx)
    piece = (MINE, CX, CROSS)
    ships = (WIDTH, SHIPS)
    return pl.pallas_call(
        spread_kernel,
        out_shape=jax.ShapeDtypeStruct((NCOL, CX, CROSS), jnp.float32),
        in_specs=[smem, hbm],
        out_specs=vmem,
        scratch_shapes=[
            pltpu.VMEM((WIDTH * 2 * MINE, CX, CROSS), jnp.float32),
            pltpu.VMEM((2 * MINE, CX, CROSS), jnp.float32),
            pltpu.VMEM(piece, jnp.float32),
            dma(ships),
            dma(ships),
            dma((SHIPS,)),
            dma((SHIPS,)),
            dma(ships),
            dma(ships),
            dma,
            dma,
            dma,
        ],
        compiler_params=pltpu.CompilerParams(
            collective_id=1, has_side_effects=True, vmem_limit_bytes=40 * 2**20
        ),
        name="spread",
    )(table, boxes)


def solution(mesh):
    placed = (P(None, "orb", None), P("orb", None), P(), P(), P())
    return jax.shard_map(
        body, mesh=mesh, in_specs=placed, out_specs=P(None, "orb", None), check_vma=False
    )
```

```python
import functools

import jax
import jax.numpy as jnp
import numpy as np
from jax import lax
from jax.experimental import pallas as pl
from jax.experimental.pallas import tpu as pltpu
from jax.sharding import PartitionSpec as P

B = 32
CX = 8
MEMBERS = 8
NCOL = 96
HALF = NCOL // 2
SLABS = 64
WIDTH = 4
CROSS = B * B
QUAD = CROSS // 4
WIN = (WIDTH + 1) * CX
MINE = 12
BATCH = 8
SLOTS = 168
PIECES = 8
PIECE = HALF // PIECES
SHIPS = 4
BOXES = MINE // SHIPS

lap_weights = (
    -5369.0 / 1800.0,
    12.0 / 7.0,
    -15.0 / 56.0,
    10.0 / 189.0,
    -1.0 / 112.0,
    2.0 / 1925.0,
    -1.0 / 16632.0,
)
stencil_reach = 6
mixing = 0.25


def halves(values):
    hi = values.astype(jnp.bfloat16).astype(np.float64)
    lo = (values - hi).astype(jnp.bfloat16).astype(np.float64)
    return hi, lo


def tables():
    idx = np.arange(1, B + 1)
    sine = np.sqrt(2.0 / (B + 1)) * np.sin(np.pi * np.outer(idx, idx) / (B + 1))
    single = 2.0 - 2.0 * np.cos(np.pi * idx / (B + 1))
    part = [sine[: B // 2, p::2] for p in (0, 1)]
    lap = np.zeros((B, B))
    for o, w in enumerate(lap_weights):
        lap += w * (np.eye(B, k=o) if o == 0 else np.eye(B, k=o) + np.eye(B, k=-o))
    flip = lap[: B // 2, ::-1][:, : B // 2]
    fold = [lap[: B // 2, : B // 2] + flip, lap[: B // 2, : B // 2] - flip]
    eye = np.eye(B // 2)
    kmat, lmat, modes = [], [], []
    for py in (0, 1):
        for pz in (0, 1):
            kmat.append(np.kron(part[py], part[pz]))
            lmat.append(-0.125 * (np.kron(fold[py], eye) + np.kron(eye, fold[pz])).T)
            cross = single[py::2][:, None] + single[pz::2][None, :]
            modes.append(single[:, None] + cross.reshape(1, -1))
    inv = (-mixing / np.concatenate(modes, axis=1)).astype(np.float32)
    ktab = np.stack(halves(np.stack(kmat))).astype(jnp.bfloat16)
    ltab = np.stack(halves(np.stack(lmat))).astype(jnp.bfloat16)
    a3 = np.zeros((CX, B, 128))
    b3 = np.zeros((CX, WIN, 128))
    lx = np.zeros((CX, WIN, 128))
    for sub in range(CX):
        placed = np.zeros((B, WIN))
        placed[:, sub : sub + B] = sine
        hi, lo = halves(placed)
        a3[sub, :, :120] = np.concatenate([hi, hi, lo], axis=1)
        b3[sub, :, :96] = np.concatenate([hi.T, hi.T, lo.T], axis=1)
        lap_placed = np.zeros((WIN, WIN))
        lap_placed[sub : sub + B, sub : sub + B] = -0.5 * lap
        hi, lo = halves(lap_placed)
        lx[sub, :, :80] = np.concatenate([hi, lo], axis=1)
    return (
        ktab,
        ltab,
        inv,
        a3.astype(np.float32),
        b3.astype(np.float32),
        lx.astype(jnp.bfloat16),
    )


def fold_lane(j, hy):
    hz, yp, zp = j // 128, j % 128 // 16, j % 16
    yl = yp if hy == 0 else 7 - yp
    return yl * B + zp + hz * (B - 1 - 2 * zp)


def folding(hy):
    j = lax.broadcasted_iota(jnp.int32, (1, QUAD), 1)
    lanes = lax.broadcasted_iota(jnp.int32, (QUAD, QUAD), 0)
    return jnp.where(lanes == fold_lane(j, hy), 1.0, 0.0).astype(jnp.bfloat16)


def unfolding(hy):
    j = lax.broadcasted_iota(jnp.int32, (QUAD, 1), 0)
    lanes = lax.broadcasted_iota(jnp.int32, (QUAD, QUAD), 1)
    return jnp.where(lanes == fold_lane(j, hy), 1.0, 0.0).astype(jnp.bfloat16)


def chunk_home(n):
    hy = n // 2
    h = n if hy == 0 else 3 - n
    return [slice((hy * 2 + hz) * QUAD + h * 128, (hy * 2 + hz) * QUAD + h * 128 + 128) for hz in (0, 1)]


def butterfly(v):
    q = [v[:, i * QUAD : (i + 1) * QUAD] for i in range(4)]
    sy0, sy1, dy0, dy1 = q[0] + q[2], q[1] + q[3], q[0] - q[2], q[1] - q[3]
    return jnp.concatenate([sy0 + sy1, sy0 - sy1, dy0 + dy1, dy0 - dy1], axis=1)


def split(v):
    hi = v.astype(jnp.bfloat16)
    lo = (v - hi.astype(jnp.float32)).astype(jnp.bfloat16)
    return hi, lo


def dot3(v, hi_mat, lo_mat):
    hi, lo = split(v)
    rows = v.shape[0]
    both = jnp.dot(
        jnp.concatenate([hi, lo], axis=0), hi_mat, preferred_element_type=jnp.float32
    )
    low = jnp.dot(hi, lo_mat, preferred_element_type=jnp.float32)
    return both[:rows] + both[rows:] + low


GROUP = 32


def prep_kernel(orb_ref, pot_ref, own_ref, planes_ref):
    fold = [folding(0), folding(1)]

    def some(g, _):
        x = orb_ref[pl.ds(g * GROUP, GROUP)].astype(jnp.float32)
        x = x.reshape(GROUP * CX, CROSS).astype(jnp.bfloat16)
        for n in range(4):
            y = jnp.dot(
                x[:, n * QUAD : (n + 1) * QUAD],
                fold[n // 2],
                preferred_element_type=jnp.float32,
            )
            for hz, lanes in enumerate(chunk_home(n)):
                part = y[:, hz * 128 : hz * 128 + 128].reshape(GROUP, CX, 128)
                own_ref[pl.ds(g * GROUP, GROUP), :, lanes] = part.astype(jnp.bfloat16)
        return 0

    lax.fori_loop(0, NCOL // GROUP, some, 0)
    rest = pot_ref[...]
    planes = []
    for _ in range(3):
        top = rest.astype(jnp.bfloat16).astype(jnp.float32)
        planes.append(top)
        rest = rest - top
    x = jnp.concatenate(planes + [jnp.zeros_like(rest)], axis=0).astype(jnp.bfloat16)
    for n in range(4):
        y = jnp.dot(
            x[:, n * QUAD : (n + 1) * QUAD], fold[n // 2], preferred_element_type=jnp.float32
        )
        for hz, lanes in enumerate(chunk_home(n)):
            for p in range(4):
                part = y[p * CX : (p + 1) * CX, hz * 128 : hz * 128 + 128]
                planes_ref[p // 2, p % 2, :, lanes] = part.astype(jnp.bfloat16)


def solve_kernel(
    idx_ref, shift_ref, partner_ref, member_ref,
    own_ref, win_ref, pot_ref, potw_ref,
    ktab_ref, ltab_ref, inv_ref, a3_ref, b3_ref, lx_ref,
    out_ref, table_ref,
    ktr_ref,
    wv, pots, acc, stg, home, listed,
):
    slab = idx_ref[0]
    core = idx_ref[1]
    def rank_colour(c, ranks):
        cl = shift_ref[c] >> 3
        a = sum(jnp.where(cl == n, rank, 0) for n, rank in enumerate(ranks))
        k = (slab - cl) & 3
        near = jnp.where(k == 0, 1, 0)
        box = (a & 1) * MINE + (a >> 1)
        t = ((k + 3) & 3) * 2 * MINE
        table_ref[c] = t + box + (box << 7) + (near << 12)
        home[jnp.where(k == 0, a, 31)] = c
        return tuple(rank + jnp.where(cl == n, 1, 0) for n, rank in enumerate(ranks))

    lax.fori_loop(0, NCOL, rank_colour, (jnp.int32(0),) * WIDTH, unroll=4)
    base = 256 - slab * CX

    count = jnp.int32(0)
    for t in range(3):
        block = slab * 3 + t

        def list_slot(p, count, t=t, block=block):
            pid = partner_ref[p, block]
            a = t * MEMBERS + member_ref[p, block]
            live = jnp.logical_and(pid >= 0, (a & 1) == core)
            pid = jnp.maximum(pid, 0)
            cj = pid >> 4
            rel = (((pid & 15) << 5) + shift_ref[cj] + base) & 511
            listed[count] = ((rel - 224) << 19) + (cj << 12) + (home[a] << 5) + a
            return count + jnp.where(live, 1, 0)

        count = lax.fori_loop(0, SLOTS // 3, list_slot, count, unroll=8)
    for extra in range(BATCH):
        listed[count + extra] = 1024 << 19

    def pair(n):
        word = listed[n]
        ci = (word >> 5) & 127
        return (word >> 1) & 15, ci, (word >> 12) & 127, shift_ref[ci] & 7, (word >> 19) - 32

    lead = idx_ref[2] * WIDTH * CX
    lead_rows = pl.ds(pl.multiple_of(lead, CX), CX)
    tail_rows = pl.ds(pl.multiple_of(WIDTH * CX - lead, CX), CX)

    def whole(planes):
        f = jnp.float32
        return planes[0, 0].astype(f) + planes[0, 1].astype(f) + planes[1, 0].astype(f)

    def widen(rows, source):
        def one(c, _):
            wv[c, rows] = source[c].astype(jnp.float32)
            return 0

        lax.fori_loop(0, NCOL, one, 0, unroll=4)

    widen(lead_rows, own_ref)
    for k in range(WIDTH):
        rows = tail_rows if k == WIDTH - 1 else slice((k + 1) * CX, (k + 2) * CX)
        widen(rows, win_ref.at[k])
    pots[lead_rows] = whole(pot_ref)
    pots[tail_rows] = whole(potw_ref.at[WIDTH - 1])
    for k in range(1, WIDTH):
        pots[k * CX : (k + 1) * CX] = whole(potw_ref.at[k - 1])
    for h in range(2):
        for q in range(4):
            ktr_ref[h, q] = ktab_ref[h, q].astype(jnp.float32).T.astype(jnp.bfloat16)

    row_ids = lax.broadcasted_iota(jnp.int32, (WIN, 1), 0)

    for group in range(2):
        for j in range(6):
            i = group * 6 + j
            c = home[2 * i + core]
            sub = shift_ref[c] % CX
            inside = jnp.logical_and(row_ids >= sub, row_ids < sub + B)
            w = jnp.where(inside, wv[c], 0.0)
            stg[j * WIN : (j + 1) * WIN] = butterfly(w)
            twice = jnp.concatenate([w, w], axis=0).astype(jnp.bfloat16)
            acc[i] = pots[...] * w + jnp.dot(
                lx_ref[sub][:, :80], twice, preferred_element_type=jnp.float32
            )
        for q in range(4):
            cols = slice(q * QUAD, (q + 1) * QUAD)
            v = stg[0 : 6 * WIN, cols]
            stg[0 : 6 * WIN, cols] = dot3(v, ltab_ref[0, q], ltab_ref[1, q])
        for j in range(6):
            i = group * 6 + j
            acc[i] = acc[i] + butterfly(stg[j * WIN : (j + 1) * WIN])

    lane_ids = lax.broadcasted_iota(jnp.int32, (1, 128), 1)
    lane_row = lane_ids - WIN * jnp.where(lane_ids >= WIN, 1, 0)
    lane_row = lane_row - WIN * jnp.where(lane_ids >= 2 * WIN, 1, 0)

    def batch(b, _):
        for p in range(BATCH):
            _, ci, cj, sub, lo = pair(b * BATCH + p)
            held = jnp.logical_and(lane_row >= lo, lane_row < lo + B)
            left = jnp.where(held, a3_ref[sub], 0.0).astype(jnp.bfloat16)
            dens = wv[ci] * wv[cj]
            hi = dens.astype(jnp.bfloat16).astype(jnp.float32)
            stack = jnp.concatenate(
                [hi, dens - hi, hi, jnp.zeros((CX, CROSS), jnp.float32)], axis=0
            ).astype(jnp.bfloat16)
            u = jnp.dot(left, stack, preferred_element_type=jnp.float32)
            stg[p * B : (p + 1) * B] = butterfly(u)
        for q in range(4):
            cols = slice(q * QUAD, (q + 1) * QUAD)
            g = dot3(stg[:, cols], ktab_ref[0, q], ktab_ref[1, q])
            g = g.reshape(BATCH, B, QUAD) * inv_ref[:, cols][None]
            g = g.reshape(BATCH * B, QUAD)
            stg[:, cols] = dot3(g, ktr_ref[0, q], ktr_ref[1, q])
        for p in range(BATCH):
            m, _, cj, sub, lo = pair(b * BATCH + p)
            held = jnp.logical_and(row_ids >= lo, row_ids < lo + B)
            right = jnp.where(held, b3_ref[sub], 0.0).astype(jnp.bfloat16)
            hi, low = split(butterfly(stg[p * B : (p + 1) * B]))
            stack = jnp.concatenate([hi, low, hi], axis=0)
            field = jnp.dot(right[:, :96], stack, preferred_element_type=jnp.float32)
            acc[m] = acc[m] + field * wv[cj]
        return 0

    lax.fori_loop(0, (count + BATCH - 1) // BATCH, batch, 0)

    for n in range(4):
        back = unfolding(n // 2)
        low_z, high_z = chunk_home(n)
        for group in range(2):
            rows = slice(group * 6, group * 6 + 6)
            v = jnp.concatenate([acc[rows, :, low_z], acc[rows, :, high_z]], axis=2)
            hi, lo = split(v.reshape(6 * WIN, QUAD))
            y = jnp.dot(
                jnp.concatenate([hi, lo], axis=0), back, preferred_element_type=jnp.float32
            )
            y = y[: 6 * WIN] + y[6 * WIN :]
            for j in range(6):
                for k in range(WIDTH + 1):
                    first = j * WIN + k * CX
                    out_ref[k, group * 6 + j, :, n * QUAD : (n + 1) * QUAD] = y[
                        first : first + CX
                    ]


def slab_at(step):
    s = lax.axis_index("orb")
    group = lax.axis_index("group")
    y, zl, zh, core = s % 4, (s // 4) % 4, group // 2, group % 2
    if step > 0:
        turn = (zl + (y + step) // 4) // 4
    else:
        turn = 1 - (zl - (1 - (y + step + 4) // 4) + 4) // 4
    return ((zh + turn) % 2 * 2 + core, (s + step + SLABS) % SLABS)


def ring(step):
    s = lax.axis_index("orb")
    return (lax.axis_index("group"), s - s % 4 + (s % 4 + step + 4) % 4)


def either(which, first, second):
    return tuple(a + which * (b - a) for a, b in zip(first, second))


def sibling():
    group = lax.axis_index("group")
    return (group // 2 * 2 + 1 - group % 2, lax.axis_index("orb"))


def greet(others):
    barrier = pltpu.get_barrier_semaphore()
    for other in others:
        pl.semaphore_signal(
            barrier, inc=1, device_id=other, device_id_type=pl.DeviceIdType.MESH
        )
    pl.semaphore_wait(barrier, len(others))


def remote(src, dst, send, recv, device):
    return pltpu.make_async_remote_copy(
        src_ref=src,
        dst_ref=dst,
        send_sem=send,
        recv_sem=recv,
        device_id=device,
        device_id_type=pl.DeviceIdType.MESH,
    )


def fetch_kernel(own, pot, win, potw, send, recv, dsend, drecv):
    core = lax.axis_index("group") % 2
    y = lax.axis_index("orb") % 4
    high, odd = y // 2, y % 2
    greet([ring(-1), ring(1), slab_at(-4), slab_at(4), sibling()])

    def mine(q):
        return pot.at[core] if q == PIECES else own.at[pl.ds(core * HALF + q * PIECE, PIECE)]

    def held(t, q):
        if q == PIECES:
            return potw.at[t, core]
        return win.at[t, pl.ds(core * HALF + q * PIECE, PIECE)]

    def move(stream, src, t, q, device):
        return remote(src, held(t, q), send.at[stream, q], recv.at[t, q], device)

    def to_sibling(t, q):
        return remote(held(t, q), held(t, q), dsend.at[t, q], drecv.at[t, q], sibling())

    relayed = 2 - 2 * odd
    onward = either(odd, ring(1), ring(-1))
    copies = {
        0: (None, lambda q: move(0, mine(q), 3, q, either(high, slab_at(-4), slab_at(4)))),
        1: (y != 3, lambda q: move(1, mine(q), 0, q, ring(-1))),
        2: (y == 3, lambda q: move(1, held(3, q), 0, q, ring(-1))),
        3: (y != 0, lambda q: move(2, mine(q), 2, q, ring(1))),
        4: (y == 0, lambda q: move(2, held(3, q), 2, q, ring(1))),
        5: (None, lambda q: move(3, held(relayed, q), 1, q, onward)),
    }

    def act(which, q, what):
        cond, make = copies[which]
        if cond is None:
            getattr(make(q), what)()
        else:

            @pl.when(cond)
            def _():
                getattr(make(q), what)()

    def arrived(t, q):
        move(0, held(t, q), t, q, sibling()).wait_recv()
        to_sibling(t, q).start()

    turns = range(PIECES + 1)
    for q in turns:
        for which in (0, 1, 3):
            act(which, q, "start")
    for q in turns:
        arrived(3, q)
        act(2, q, "start")
        act(4, q, "start")
        arrived(relayed, q)
        act(5, q, "start")
    for q in turns:
        arrived(2 - relayed, q)
    for q in turns:
        arrived(1, q)
    for q in turns:
        for which in range(6):
            act(which, q, "wait_send")
        for t in range(WIDTH):
            to_sibling(t, q).wait()


def spread_kernel(
    table_ref, boxes, out, got, ext, stage,
    send, recv, rsend, rrecv, dsend, drecv, osend, orecv, ksem,
):
    core = lax.axis_index("group") % 2
    slab = lax.axis_index("orb")
    y = slab % 4
    high, odd = y // 2, y % 2
    greet(
        [ring(-1), ring(1), slab_at(-4), slab_at(4), slab_at(-3), slab_at(3), sibling()]
    )

    def part(q):
        return pl.ds(q * BOXES, BOXES)

    def landing(t, q):
        return got.at[pl.ds((t * 2 + core) * MINE + q * BOXES, BOXES)]

    def ship(t, src, q, device):
        return remote(src, landing(t, q), send.at[t, q], recv.at[t, q], device)

    low_cross = (y % 2) * (1 - high)
    high_cross = (1 - y % 2) * high
    to_one = either(high_cross, ring(1), slab_at(-3))
    to_three = either(low_cross, ring(-1), slab_at(3))
    to_z = either(high, slab_at(4), slab_at(-4))
    outer = WIDTH * (1 - high)
    inner = WIDTH * high

    def by_z(q):
        return ship(3, boxes.at[outer, part(q)], q, to_z)

    def by_one(q):
        return ship(0, boxes.at[1, part(q)], q, to_one)

    def by_three(q):
        return ship(2, boxes.at[3, part(q)], q, to_three)

    def to_relay(q):
        return remote(
            boxes.at[2, part(q)],
            stage.at[part(q)],
            rsend.at[q],
            rrecv.at[q],
            either(odd, ring(1), ring(-1)),
        )

    def relay(q):
        return ship(1, stage.at[part(q)], q, either(odd, ring(-1), ring(1)))

    def to_sibling(t, q):
        here = landing(t, q)
        return remote(here, here, dsend.at[t, q], drecv.at[t, q], sibling())

    def arrived(t, q):
        ship(t, boxes.at[0, part(q)], q, sibling()).wait_recv()
        to_sibling(t, q).start()

    local = remote(boxes.at[inner], ext.at[pl.ds(core * MINE, MINE)], osend, orecv, sibling())
    for q in range(SHIPS):
        to_relay(q).start()
    for q in range(SHIPS):
        by_z(q).start()
        by_one(q).start()
        by_three(q).start()
    local.start()
    keep = pltpu.make_async_copy(boxes.at[inner], ext.at[pl.ds(core * MINE, MINE)], ksem)
    keep.start()
    for q in range(SHIPS):
        to_relay(q).wait_recv()
        relay(q).start()
    for q in range(SHIPS):
        arrived(3, q)
        arrived(0, q)
        arrived(2, q)
    for q in range(SHIPS):
        arrived(1, q)
    local.wait()
    keep.wait()
    for q in range(SHIPS):
        to_relay(q).wait_send()
        for copy in (by_z(q), by_one(q), by_three(q), relay(q)):
            copy.wait_send()
        for t in range(WIDTH):
            to_sibling(t, q).wait()

    def place(c, _):
        word = table_ref[c]
        extra = jnp.where((word >> 12) == 1, 1.0, 0.0)
        out[c] = got[word & 127] + extra * ext[(word >> 7) & 31]
        return 0

    lax.fori_loop(0, NCOL, place, 0, unroll=8)


def body(orbitals, potential, box_shift, pair_partner, pair_member):
    ktab, ltab, inv, a3, b3, lx = tables()
    place = lax.axis_index("orb").astype(jnp.int32)
    high = place % 4 // 2
    slab = (place - 4 * high) % SLABS
    core = lax.axis_index("group").astype(jnp.int32) % 2
    smem = pl.BlockSpec(memory_space=pltpu.SMEM)
    vmem = pl.BlockSpec(memory_space=pltpu.VMEM)
    hbm = pl.BlockSpec(memory_space=pltpu.HBM)
    dma = pltpu.SemaphoreType.DMA
    own, pot = pl.pallas_call(
        prep_kernel,
        out_shape=(
            jax.ShapeDtypeStruct((NCOL, CX, CROSS), jnp.bfloat16),
            jax.ShapeDtypeStruct((2, 2, CX, CROSS), jnp.bfloat16),
        ),
        in_specs=[vmem] * 2,
        out_specs=(vmem, vmem),
        compiler_params=pltpu.CompilerParams(vmem_limit_bytes=16 * 2**20),
        name="prep",
    )(orbitals, potential)
    streams = (WIDTH, PIECES + 1)
    win, potw = pl.pallas_call(
        fetch_kernel,
        out_shape=(
            jax.ShapeDtypeStruct((WIDTH, NCOL, CX, CROSS), jnp.bfloat16),
            jax.ShapeDtypeStruct((WIDTH, 2, 2, CX, CROSS), jnp.bfloat16),
        ),
        in_specs=[hbm] * 2,
        out_specs=(hbm, hbm),
        scratch_shapes=[dma(streams)] * 4,
        compiler_params=pltpu.CompilerParams(
            collective_id=0, has_side_effects=True, vmem_limit_bytes=2 * 2**20
        ),
        name="fetch",
    )(own, pot)
    idx = jnp.stack([slab, core, high])
    boxes, table = pl.pallas_call(
        solve_kernel,
        out_shape=(
            jax.ShapeDtypeStruct((WIDTH + 1, MINE, CX, CROSS), jnp.float32),
            jax.ShapeDtypeStruct((NCOL,), jnp.int32),
        ),
        in_specs=[smem] * 4 + [vmem] * 10,
        out_specs=(vmem, smem),
        scratch_shapes=[
            pltpu.VMEM((2, 4, QUAD, QUAD), jnp.bfloat16),
            pltpu.VMEM((NCOL, WIN, CROSS), jnp.float32),
            pltpu.VMEM((WIN, CROSS), jnp.float32),
            pltpu.VMEM((MINE, WIN, CROSS), jnp.float32),
            pltpu.VMEM((BATCH * B, CROSS), jnp.float32),
            pltpu.SMEM((32,), jnp.int32),
        ]
        + [pltpu.SMEM((SLOTS + BATCH,), jnp.int32)],
        compiler_params=pltpu.CompilerParams(vmem_limit_bytes=40 * 2**20),
        name="solve",
    )(idx, box_shift, pair_partner.T, pair_member.T, own, win, pot, potw, ktab, ltab, inv, a3, b3, lx)
    piece = (MINE, CX, CROSS)
    ships = (WIDTH, SHIPS)
    return pl.pallas_call(
        spread_kernel,
        out_shape=jax.ShapeDtypeStruct((NCOL, CX, CROSS), jnp.float32),
        in_specs=[smem, hbm],
        out_specs=vmem,
        scratch_shapes=[
            pltpu.VMEM((WIDTH * 2 * MINE, CX, CROSS), jnp.float32),
            pltpu.VMEM((2 * MINE, CX, CROSS), jnp.float32),
            pltpu.VMEM(piece, jnp.float32),
            dma(ships),
            dma(ships),
            dma((SHIPS,)),
            dma((SHIPS,)),
            dma(ships),
            dma(ships),
            dma,
            dma,
            dma,
        ],
        compiler_params=pltpu.CompilerParams(
            collective_id=1, has_side_effects=True, vmem_limit_bytes=40 * 2**20
        ),
        name="spread",
    )(table, boxes)


def solution(mesh):
    placed = (P(None, "orb", None), P("orb", None), P(), P(), P())
    return jax.shard_map(
        body, mesh=mesh, in_specs=placed, out_specs=P(None, "orb", None), check_vma=False
    )
```
